32 devices in a mesh: depth: 4 (over z), rows: 8 (over y, x, core).
Axes of the slice: x: 2, y: 2, z: 4, core: 2. Of those that a mesh axis runs over, the one named last changes fastest.
Arguments:
- target: float32 [4, 2, 4096, 4096], P('depth', None, 'rows'), may hold values from -6 to 6
- depth_index: int32 [4], P('depth'), may hold values from 0 to 255
- band_mask: int32 [4, 2, 4096], P('depth'), may hold values from 0 to 1, as said below
Outputs:
- hologram: float32 [2, 4096, 4096], P(None, ('depth', 'rows'))
The draws below stay inside these ranges and needn't reach their ends.
Inputs may be any that keep to these rules, and one draw needn't show every extreme that they name: `band_mask`: for each plane and each of the two dimensions, the ones are exactly the frequency indices k with min(k, 4096 - k) below a cutoff between 512 and 2048.
All inputs are finite; a program needn't handle non-finite values.
Results may differ from the reference program's by a relative error of at most 0.0009.
Values sent between devices are 32-bit elements; how exact they have to be, the bound alone decides.
A program may use at most 128 MiB of HBM per device.

```python
import math
import jax
import jax.numpy as jnp
from jax import lax

N = 4096
PLANES = 4
DEPTHS = 256


def draw_band_mask(key, part):
    cutoff = jax.random.randint(key, (PLANES, 2, 1), N // 8, N // 2 + 1)
    indices = jnp.arange(N, dtype=jnp.int32)
    folded = jnp.minimum(indices, N - indices)
    return (folded[None, None, :] < cutoff).astype(jnp.int32)


def place_ends(values, key, low, top_value):
    spot = [jax.random.randint(jax.random.fold_in(key, axis), (), 0, length) for axis, length in enumerate(values.shape)]
    main_axis = values.shape.index(max(values.shape))
    neighbour = spot[:main_axis] + [(spot[main_axis] + 1) % values.shape[main_axis]] + spot[main_axis + 1:]
    return values.at[tuple(spot)].set(low).at[tuple(neighbour)].set(top_value)


def levels(stream_key, dims, cuts, low, top_value):
    loudness = 1.0
    for axis_at, parts in cuts:
        steps = jax.random.uniform(jax.random.fold_in(jax.random.fold_in(stream_key, 6), axis_at), (parts,), jnp.float32, low / len(cuts), top_value / len(cuts))
        loudness = loudness * jnp.repeat(jnp.exp(steps), dims[axis_at] // parts).reshape((-1,) + (1,) * (len(dims) - 1 - axis_at))
    return loudness


def normal_values(key, dims, width, reach, split=(), kind=jnp.bfloat16):
    result = jax.random.normal(key, dims, jnp.float32) * width
    if len(split) > 0:
        result = levels(key, dims, split, -0.22, 0.18) * result
    return jnp.clip(result, min=-reach, max=reach).astype(kind)


def setup_inputs(seed: int = 0) -> dict:
    key_of = jax.random.split(jax.random.key(seed), 4)
    return {
        "target": normal_values(key_of[0], (PLANES, 2, N, N), 1.0, 6.0, ((0, 4), (2, 8)), jnp.float32),
        "depth_index": place_ends(jax.random.randint(key_of[1], (PLANES,), 0, DEPTHS), jax.random.fold_in(key_of[1], 1), 0, DEPTHS - 1).astype(jnp.int32),
        "band_mask": draw_band_mask(jax.random.fold_in(key_of[3], 71), 0),
    }


def reference(target, depth_index, band_mask):
    planes_all = target.shape[0]
    indices = jnp.arange(N, dtype=jnp.int32)
    signed = jnp.where(indices < N // 2, indices, indices - N)
    frequency = signed.astype(jnp.float32) / N
    radical = jnp.sqrt(4.0 - frequency[:, None] ** 2 - frequency[None, :] ** 2)

    def add_plane(running_sum, inputs):
        plane_data, level_index, mask_pair = inputs
        wavefront = lax.complex(plane_data[0], plane_data[1])
        spectrum = jnp.fft.fft2(wavefront, norm='ortho')
        distance = 100.0 + 2.0 * level_index.astype(jnp.float32)
        phases = 2.0 * math.pi * distance * (radical - 2.0)
        weights = mask_pair[0].astype(jnp.float32)[:, None] * mask_pair[1].astype(jnp.float32)[None, :]
        rotated = spectrum * lax.complex(jnp.cos(phases) * weights, jnp.sin(phases) * weights)
        return (running_sum + rotated, None)
    zeros_real = jnp.zeros((N, N), dtype=jnp.float32)
    initial = lax.complex(zeros_real, zeros_real)
    summed, _ = lax.scan(add_plane, initial, (target, depth_index, band_mask))
    field_out = jnp.fft.ifft2(summed, norm='ortho') / jnp.sqrt(jnp.float32(planes_all))
    return jnp.stack([jnp.real(field_out), jnp.imag(field_out)]).astype(jnp.float32)
```

```python
import functools
import math

import jax
import jax.numpy as jnp
import numpy as np
from jax import lax
from jax.experimental import pallas as pl
from jax.experimental.pallas import tpu as pltpu
from jax.sharding import PartitionSpec as P


LOW = 32
HIGH = 128
N = LOW * HIGH
VMEM_LIMIT = 56 * 1024 * 1024


def scaled(value, factor_real, factor_imaginary):
    real, imaginary = value
    if abs(factor_imaginary) < 1e-12:
        if factor_real > 0:
            return (real, imaginary)
        return (-real, -imaginary)
    if abs(factor_real) < 1e-12:
        if factor_imaginary > 0:
            return (-imaginary, real)
        return (imaginary, -real)
    a, b = np.float32(factor_real), np.float32(factor_imaginary)
    return (real * a - imaginary * b, real * b + imaginary * a)


def root(numerator, length, direction):
    angle = direction * 2.0 * math.pi * (numerator % length) / length
    return math.cos(angle), math.sin(angle)


def add(left, right):
    return (left[0] + right[0], left[1] + right[1])


def subtract(left, right):
    return (left[0] - right[0], left[1] - right[1])


def butterfly(values, direction):
    count = len(values)
    if count == 1:
        return values
    even = butterfly(values[0::2], direction)
    odd = butterfly(values[1::2], direction)
    odd = [scaled(v, *root(k, count, direction)) for k, v in enumerate(odd)]
    return [add(e, o) for e, o in zip(even, odd)] + [subtract(e, o) for e, o in zip(even, odd)]


def dense_table(direction):
    index = np.arange(HIGH)
    angles = direction * 2.0 * np.pi / HIGH * (index[:, None] * index[None, :] % HIGH)
    cosine, sine = np.cos(angles), np.sin(angles)
    return np.block([[cosine, -sine], [sine, cosine]])


def halves(table):
    high = table.astype(np.float32).astype(jnp.bfloat16)
    low = (table - high.astype(np.float64)).astype(np.float32).astype(jnp.bfloat16)
    return jnp.asarray(high), jnp.asarray(low)


def twiddles(direction, scaling):
    product = np.arange(LOW)[:, None] * np.arange(HIGH)[None, :] % N
    angles = direction * 2.0 * np.pi / N * product
    return (
        jnp.asarray((np.cos(angles) * scaling).astype(np.float32)),
        jnp.asarray((np.sin(angles) * scaling).astype(np.float32)),
    )


def split(value):
    high = value.astype(jnp.bfloat16)
    return high, (value - high.astype(jnp.float32)).astype(jnp.bfloat16)


def tripled(value):
    high, low = split(value)
    return jnp.concatenate([high, low, high], axis=0)


def dot(left, right):
    return jnp.dot(left, right, preferred_element_type=jnp.float32)


def width_kernel(chunk, chunks, owners, x_ref, tr_ref, ti_ref, th_ref, tl_ref, o_ref, hi_ref, lo_ref):
    tile = x_ref.shape[1]

    def body(step, carry):
        rows = pl.ds(pl.multiple_of(step * 16, 16), 16)
        values = []
        for first in range(owners):
            total = None
            for second in range(chunks):
                at = (first + owners * second) * HIGH
                value = (x_ref[0, rows, at:at + HIGH], x_ref[1, rows, at:at + HIGH])
                value = scaled(value, *root(chunk * second, chunks, -1.0))
                total = value if total is None else add(total, value)
            values.append(scaled(total, *root(chunk * first, LOW, -1.0)))
        for owner, (real, imaginary) in enumerate(butterfly(values, -1.0)):
            k = chunks * owner + chunk
            turn_real, turn_imaginary = tr_ref[k:k + 1, :], ti_ref[k:k + 1, :]
            high, low = split(real * turn_real - imaginary * turn_imaginary)
            hi_ref[owner, rows, :HIGH] = high
            lo_ref[owner, rows, :HIGH] = low
            high, low = split(real * turn_imaginary + imaginary * turn_real)
            hi_ref[owner, rows, HIGH:] = high
            lo_ref[owner, rows, HIGH:] = low
        return carry

    lax.fori_loop(0, tile // 16, body, 0)
    for owner in range(owners):
        high = hi_ref[owner]
        out = dot(high, th_ref[...]) + dot(lo_ref[owner], th_ref[...]) + dot(high, tl_ref[...])
        o_ref[owner, 0] = out[:, :HIGH]
        o_ref[owner, 1] = out[:, HIGH:]


def along_width(field, chunk, chunks, owners, tables):
    _, height, _ = field.shape
    tile = min(128, height)
    whole = lambda a: pl.BlockSpec(a.shape, lambda i: (0,) * a.ndim)
    return pl.pallas_call(
        functools.partial(width_kernel, chunk, chunks, owners),
        grid=(height // tile,),
        in_specs=[pl.BlockSpec((2, tile, N), lambda i: (0, i, 0))] + [whole(a) for a in tables],
        out_specs=pl.BlockSpec((owners, 2, tile, HIGH), lambda i: (0, 0, i, 0)),
        out_shape=jax.ShapeDtypeStruct((owners, 2, height, HIGH), jnp.float32),
        scratch_shapes=[pltpu.VMEM((owners, tile, 2 * HIGH), jnp.bfloat16)] * 2,
        compiler_params=pltpu.CompilerParams(vmem_limit_bytes=VMEM_LIMIT),
        cost_estimate=pl.CostEstimate(flops=6 * height * HIGH * HIGH * 4 * owners * 2, bytes_accessed=field.size * 4 + field.size * 4 // chunks, transcendentals=0),
    )(field, *tables)


def series(values, points):
    nodes = np.cos(np.pi * (np.arange(400) + 0.5) / 400) * 0.125 + 0.125
    basis = np.polynomial.chebyshev.Chebyshev.fit(nodes, values(np.sqrt(nodes)), points, domain=[0.0, 0.25])
    return [np.float32(c) for c in basis.convert(kind=np.polynomial.Polynomial).coef]


COSINE = series(lambda r: np.cos(2.0 * np.pi * r), 6)
SINE = series(lambda r: np.sin(2.0 * np.pi * r) / r, 6)


def horner(coefficients, at):
    total = coefficients[-1]
    for c in coefficients[-2::-1]:
        total = total * at + c
    return total


def signed(natural):
    return jnp.where(natural < N // 2, natural, natural - N).astype(jnp.float32)


def column_kernel(scalars_ref, x_ref, tr_ref, ti_ref, f_ref, i_ref, o_ref, work_ref):
    owners, _, pieces, _, _ = x_ref.shape
    distance = scalars_ref[0].astype(jnp.float32) * 2.0 + 100.0
    limit_height = scalars_ref[1].astype(jnp.float32)
    limit_width = scalars_ref[2].astype(jnp.float32)
    column = scalars_ref[3]

    def forward(step, carry):
        rows = pl.ds(pl.multiple_of(step * 8, 8), 8)
        low_rows = pl.ds(pl.multiple_of(step * 8 + HIGH, 8), 8)
        values = [(x_ref[s, 0, p, rows, :], x_ref[s, 1, p, rows, :]) for s in range(owners) for p in range(pieces)]
        for k, (real, imaginary) in enumerate(butterfly(values, -1.0)):
            work_ref[k, rows, :] = real
            work_ref[k, low_rows, :] = imaginary
        return carry

    lax.fori_loop(0, HIGH // 8, forward, 0)

    across = signed(lax.broadcasted_iota(jnp.int32, (1, HIGH), 1) * LOW + column)
    inside_width = jnp.abs(across) < limit_width
    across_square = (across * (1.0 / N)) ** 2

    def turned(k):
        real, imaginary = work_ref[k, :HIGH, :], work_ref[k, HIGH:, :]
        turn_real, turn_imaginary = tr_ref[k], ti_ref[k]
        return jnp.concatenate(
            [real * turn_real - imaginary * turn_imaginary, real * turn_imaginary + imaginary * turn_real], axis=0
        )

    def propagate(k, real, imaginary):
        down = signed(lax.broadcasted_iota(jnp.int32, (HIGH, HIGH), 0) * LOW + k)
        square = (down * (1.0 / N)) ** 2 + across_square
        rest_square = 4.0 - square
        drop = 2.0 - rest_square * lax.rsqrt(rest_square)
        turns = -distance * (0.25 * (square + drop * drop))
        rest = turns - jnp.floor(turns + 0.5)
        at = rest * rest
        keep = jnp.logical_and(jnp.abs(down) < limit_height, inside_width)
        cosine = jnp.where(keep, horner(COSINE, at), 0.0)
        sine = jnp.where(keep, horner(SINE, at) * rest, 0.0)
        return jnp.concatenate([real * cosine - imaginary * sine, real * sine + imaginary * cosine], axis=0)

    def middle(step, carry):
        pair = [2 * step, 2 * step + 1]
        spectrum = dot(f_ref[...], tripled(jnp.concatenate([turned(k) for k in pair], axis=1)))
        moved = [
            propagate(k, spectrum[:HIGH, i * HIGH:(i + 1) * HIGH], spectrum[HIGH:, i * HIGH:(i + 1) * HIGH])
            for i, k in enumerate(pair)
        ]
        back = dot(i_ref[...], tripled(jnp.concatenate(moved, axis=1)))
        for i, k in enumerate(pair):
            real, imaginary = back[:HIGH, i * HIGH:(i + 1) * HIGH], back[HIGH:, i * HIGH:(i + 1) * HIGH]
            turn_real, turn_imaginary = tr_ref[k], ti_ref[k]
            work_ref[k, :HIGH, :] = real * turn_real + imaginary * turn_imaginary
            work_ref[k, HIGH:, :] = imaginary * turn_real - real * turn_imaginary
        return carry

    lax.fori_loop(0, LOW // 2, middle, 0)

    def inverse(step, carry):
        rows = pl.ds(pl.multiple_of(step * 8, 8), 8)
        low_rows = pl.ds(pl.multiple_of(step * 8 + HIGH, 8), 8)
        values = [(work_ref[k, rows, :], work_ref[k, low_rows, :]) for k in range(LOW)]
        for j, (real, imaginary) in enumerate(butterfly(values, 1.0)):
            o_ref[j, 0, rows, :] = real
            o_ref[j, 1, rows, :] = imaginary
        return carry

    lax.fori_loop(0, HIGH // 8, inverse, 0)


def columns_step(received, scalars, tables):
    owners, _, height, _ = received.shape
    received = received.reshape(owners, 2, height // HIGH, HIGH, HIGH)
    vmem = pl.BlockSpec(memory_space=pltpu.VMEM)
    return pl.pallas_call(
        column_kernel,
        in_specs=[pl.BlockSpec(memory_space=pltpu.SMEM)] + [vmem] * (1 + len(tables)),
        out_specs=vmem,
        out_shape=jax.ShapeDtypeStruct((LOW, 2, HIGH, HIGH), jnp.float32),
        scratch_shapes=[pltpu.VMEM((LOW, 2 * HIGH, HIGH), jnp.float32)],
        compiler_params=pltpu.CompilerParams(vmem_limit_bytes=VMEM_LIMIT),
        cost_estimate=pl.CostEstimate(flops=12 * LOW * HIGH * 256 * 256 * 2, bytes_accessed=16 * 1024 * 1024, transcendentals=0),
    )(scalars, received, *tables)


def output_kernel(chunks, *refs):
    inputs = refs[:chunks]
    tr_ref, ti_ref, th_ref, tl_ref, o_ref, work_ref = refs[chunks:]
    owners, _, height, _ = inputs[0].shape
    for owner in range(owners):
        for chunk in range(chunks):
            k = chunks * owner + chunk
            value = jnp.concatenate([inputs[chunk][owner, 0], inputs[chunk][owner, 1]], axis=1)
            high, low = split(value)
            out = dot(high, th_ref[...]) + dot(low, th_ref[...]) + dot(high, tl_ref[...])
            real, imaginary = out[:, :HIGH], out[:, HIGH:]
            turn_real, turn_imaginary = tr_ref[k:k + 1, :], ti_ref[k:k + 1, :]
            work_ref[k, 0] = real * turn_real - imaginary * turn_imaginary
            work_ref[k, 1] = real * turn_imaginary + imaginary * turn_real

    def body(step, carry):
        rows = pl.ds(pl.multiple_of(step * 8, 8), 8)
        values = [(work_ref[k, 0, rows, :], work_ref[k, 1, rows, :]) for k in range(LOW)]
        for j, (real, imaginary) in enumerate(butterfly(values, 1.0)):
            o_ref[0, rows, j * HIGH:(j + 1) * HIGH] = real
            o_ref[1, rows, j * HIGH:(j + 1) * HIGH] = imaginary
        return carry

    lax.fori_loop(0, height // 8, body, 0)


def inverse_width(parts, tables):
    height = parts[0].shape[2]
    vmem = pl.BlockSpec(memory_space=pltpu.VMEM)
    return pl.pallas_call(
        functools.partial(output_kernel, len(parts)),
        in_specs=[vmem] * (len(parts) + len(tables)),
        out_specs=vmem,
        out_shape=jax.ShapeDtypeStruct((2, height, N), jnp.float32),
        scratch_shapes=[pltpu.VMEM((LOW, 2, height, HIGH), jnp.float32)],
        compiler_params=pltpu.CompilerParams(vmem_limit_bytes=VMEM_LIMIT),
        cost_estimate=pl.CostEstimate(flops=6 * LOW * height * 256 * 256, bytes_accessed=8 * height * N * 2, transcendentals=0),
        name="output",
    )(*parts, *tables)


def local(target, depth_index, band_mask):
    owners, depths = lax.axis_size("rows"), lax.axis_size("depth")
    chunks = LOW // owners
    field = target.reshape(target.shape[1:])
    scale = 1.0 / math.sqrt(N)
    forward, backward = dense_table(-1.0), dense_table(1.0)
    left = tuple(jnp.concatenate([h, h, l], axis=1) for h, l in (halves(forward), halves(backward)))
    forward_right, backward_right = halves(forward.T), halves(backward.T)
    turn = twiddles(-1.0, scale)
    turn_back = twiddles(1.0, scale / math.sqrt(depths))
    spread = tuple(jnp.broadcast_to(t[:, :, None], (LOW, HIGH, HIGH)) for t in turn)
    limits = (jnp.sum(band_mask[0], axis=-1) + 1) // 2
    me = lax.axis_index("rows")
    rows = N // (owners * depths)

    pieces = []
    for chunk in range(chunks):
        sent = along_width(field, chunk, chunks, owners, turn + forward_right)
        received = lax.all_to_all(sent, "rows", split_axis=0, concat_axis=0, tiled=True)
        scalars = jnp.stack([depth_index[0], limits[0], limits[1], me * chunks + chunk]).astype(jnp.int32)
        part = columns_step(received, scalars, spread + left)
        pieces.append(lax.psum_scatter(part, "depth", scatter_dimension=0, tiled=True))
    results = []
    for share in pieces:
        share = share.reshape(share.shape[0], 2, HIGH // rows, rows, HIGH)
        share = jnp.transpose(share, (0, 2, 1, 3, 4)).reshape(owners, 2, rows, HIGH)
        results.append(lax.all_to_all(share, "rows", split_axis=0, concat_axis=0, tiled=True))
    return inverse_width(results, turn_back + backward_right)


MESH = pl.DeviceIdType.MESH
PART = 32
PARTS = HIGH // PART
AHEAD = 3


def slots():
    half = PART // 2
    order = []
    for part in range(PARTS):
        order += list(range(half * part, half * (part + 1)))
        order += list(range(HIGH - half * (part + 1), HIGH - half * part))
    return np.array(order)


def both(index):
    return np.concatenate([index, index + HIGH])


def nt_dot(left, right):
    return lax.dot_general(left, right, (((1,), (1,)), ((), ())), preferred_element_type=jnp.float32)


def spread_kernel(chunks, x_ref, tr_ref, ti_ref, th_ref, tl_ref, o_ref, work_ref):
    def body(step, carry):
        rows = pl.ds(pl.multiple_of(step * 8, 8), 8)
        values = [(x_ref[0, rows, g * HIGH:(g + 1) * HIGH], x_ref[1, rows, g * HIGH:(g + 1) * HIGH]) for g in range(LOW)]
        for k, (real, imaginary) in enumerate(butterfly(values, -1.0)):
            turn_real, turn_imaginary = tr_ref[k:k + 1, :], ti_ref[k:k + 1, :]
            work_ref[k, rows, :HIGH] = real * turn_real - imaginary * turn_imaginary
            work_ref[k, rows, HIGH:] = real * turn_imaginary + imaginary * turn_real
        return carry

    lax.fori_loop(0, HIGH // 8, body, 0)

    def dense(step, carry):
        value = jnp.concatenate([work_ref[2 * step], work_ref[2 * step + 1]], axis=0)
        high, low = split(value)
        out = nt_dot(th_ref[...], high) + nt_dot(th_ref[...], low) + nt_dot(tl_ref[...], high)
        for i in range(2):
            k = 2 * step + i
            owner, chunk = k // chunks, k % chunks
            for part in range(PARTS):
                for side in range(2):
                    at = side * HIGH + part * PART
                    o_ref[chunk * PARTS + part, owner, 0, side] = out[at:at + PART, i * HIGH:(i + 1) * HIGH]
        return carry

    lax.fori_loop(0, LOW // 2, dense, 0)


def spread_width(field, chunks, owners, tables):
    _, height, _ = field.shape
    whole = lambda a: pl.BlockSpec(a.shape, lambda i: (0,) * a.ndim)
    shape = (chunks * PARTS, owners, height // HIGH, 2, PART, HIGH)
    return pl.pallas_call(
        functools.partial(spread_kernel, chunks),
        grid=(height // HIGH,),
        in_specs=[pl.BlockSpec((2, HIGH, N), lambda i: (0, i, 0))] + [whole(a) for a in tables],
        out_specs=pl.BlockSpec(shape[:2] + (1,) + shape[3:], lambda i: (0, 0, i, 0, 0, 0)),
        out_shape=jax.ShapeDtypeStruct(shape, jnp.float32),
        scratch_shapes=[pltpu.VMEM((LOW, HIGH, 2 * HIGH), jnp.float32)],
        compiler_params=pltpu.CompilerParams(vmem_limit_bytes=VMEM_LIMIT),
        name="spread",
    )(field, *tables)


def line_kernel(chunks, owners, depths, scalars_ref, tr_ref, ti_ref, fh_ref, fl_ref, ih_ref, il_ref, sent_ref, back_ref,
                buf, rbuf, lbuf, work_ref, self_f, send_f, recv_f, send_r, recv_r, send_l, recv_l, self_b, send_b, recv_b):
    total = chunks * PARTS
    block = LOW // depths
    pieces = LOW // owners
    here, me = lax.axis_index("depth"), lax.axis_index("rows")
    last = depths - 1 - here

    barrier = pltpu.get_barrier_semaphore()
    for step in range(1, owners):
        pl.semaphore_signal(barrier, inc=1, device_id=(here, (me + step) % owners), device_id_type=MESH)

    @pl.when(here > 0)
    def _():
        pl.semaphore_signal(barrier, inc=1, device_id=(here - 1, me), device_id_type=MESH)

    @pl.when(last > 0)
    def _():
        pl.semaphore_signal(barrier, inc=1, device_id=(here + 1, me), device_id_type=MESH)

    pl.semaphore_wait(barrier, owners - 1 + jnp.minimum(here, 1) + jnp.minimum(last, 1))

    def own_copy(t):
        return pltpu.make_async_copy(sent_ref.at[t, me], buf.at[t, pl.ds(me * pieces, pieces)], self_f.at[t])

    def start_forward(t):
        own_copy(t).start()
        for step in range(1, owners):
            peer = (me + step) % owners
            pltpu.make_async_remote_copy(
                src_ref=sent_ref.at[t, peer],
                dst_ref=buf.at[t, pl.ds(me * pieces, pieces)],
                send_sem=send_f.at[t],
                recv_sem=recv_f.at[t],
                device_id=(here, peer),
                device_id_type=MESH,
            ).start()

    def others(t, sem):
        some = buf.at[t, pl.ds(0, pieces * (owners - 1))]
        return pltpu.make_async_copy(some, some, sem.at[t])

    def right_copy(t, q):
        return pltpu.make_async_remote_copy(
            src_ref=buf.at[t, pl.ds(q * block, block)],
            dst_ref=rbuf.at[t, q - 1],
            send_sem=send_r.at[t, q - 1],
            recv_sem=recv_r.at[t, q - 1],
            device_id=(here + 1, me),
            device_id_type=MESH,
        )

    def left_copy(t, q):
        return pltpu.make_async_remote_copy(
            src_ref=buf.at[t, pl.ds(q * block, block)],
            dst_ref=lbuf.at[t, q],
            send_sem=send_l.at[t, q],
            recv_sem=recv_l.at[t, q],
            device_id=(here - 1, me),
            device_id_type=MESH,
        )

    def final_copy(t, peer):
        return pltpu.make_async_remote_copy(
            src_ref=buf.at[t, here * block + peer],
            dst_ref=back_ref.at[t, me],
            send_sem=send_b.at[t],
            recv_sem=recv_b.at[t],
            device_id=(here, peer),
            device_id_type=MESH,
        )

    def final_own(t):
        return pltpu.make_async_copy(buf.at[t, here * block + me], back_ref.at[t, me], self_b.at[t])

    def finals(t, sem):
        some = back_ref.at[t, pl.ds(0, owners - 1)]
        return pltpu.make_async_copy(some, some, sem.at[t])

    distance = scalars_ref[0].astype(jnp.float32) * 2.0 + 100.0
    limit_height = scalars_ref[1].astype(jnp.float32)
    limit_width = scalars_ref[2].astype(jnp.float32)

    def columns(t):
        def forward(step, carry):
            rows = pl.ds(pl.multiple_of(step * 8, 8), 8)
            values = [(buf[t, p, 0, rows, :], buf[t, p, 1, rows, :]) for p in range(LOW)]
            for k, (real, imaginary) in enumerate(butterfly(values, -1.0)):
                work_ref[k, 0, rows, :] = real
                work_ref[k, 1, rows, :] = imaginary
            return carry

        lax.fori_loop(0, PART // 8, forward, 0)

        column = me * chunks + t // PARTS
        part = t % PARTS
        half = PART // 2
        slot = lax.broadcasted_iota(jnp.int32, (PART, HIGH), 0)
        turn = jnp.where(slot < half, half * part + slot, slot - half - half * (part + 1))
        across = (column + LOW * turn).astype(jnp.float32)
        inside_width = jnp.abs(across) < limit_width
        across_square = (across * (1.0 / N)) ** 2
        lanes = lax.broadcasted_iota(jnp.int32, (1, HIGH), 1) * LOW
        group = 8

        def middle(step, carry):
            taken = []
            for i in range(group):
                k = group * step + i
                real, imaginary = work_ref[k, 0], work_ref[k, 1]
                turn_real, turn_imaginary = tr_ref[pl.ds(k, 1), :], ti_ref[pl.ds(k, 1), :]
                taken.append(jnp.concatenate(
                    [real * turn_real - imaginary * turn_imaginary, real * turn_imaginary + imaginary * turn_real], axis=1))
            high, low = split(jnp.concatenate(taken, axis=0))
            spectrum = dot(high, fh_ref[...]) + dot(low, fh_ref[...]) + dot(high, fl_ref[...])
            moved = []
            for i in range(group):
                real, imaginary = spectrum[i * PART:(i + 1) * PART, :HIGH], spectrum[i * PART:(i + 1) * PART, HIGH:]
                down = signed(lanes + (group * step + i))
                square = (down * (1.0 / N)) ** 2 + across_square
                rest_square = 4.0 - square
                drop = 2.0 - rest_square * lax.rsqrt(rest_square)
                turns = -distance * (0.25 * (square + drop * drop))
                rest = turns - jnp.floor(turns + 0.5)
                at = rest * rest
                keep = jnp.logical_and(jnp.abs(down) < limit_height, inside_width)
                cosine = jnp.where(keep, horner(COSINE, at), 0.0)
                sine = jnp.where(keep, horner(SINE, at) * rest, 0.0)
                moved.append(jnp.concatenate([real * cosine - imaginary * sine, real * sine + imaginary * cosine], axis=1))
            high, low = split(jnp.concatenate(moved, axis=0))
            back = dot(high, ih_ref[...]) + dot(low, ih_ref[...]) + dot(high, il_ref[...])
            for i in range(group):
                k = group * step + i
                real, imaginary = back[i * PART:(i + 1) * PART, :HIGH], back[i * PART:(i + 1) * PART, HIGH:]
                turn_real, turn_imaginary = tr_ref[pl.ds(k, 1), :], ti_ref[pl.ds(k, 1), :]
                work_ref[k, 0] = real * turn_real + imaginary * turn_imaginary
                work_ref[k, 1] = imaginary * turn_real - real * turn_imaginary
            return carry

        lax.fori_loop(0, LOW // group, middle, 0)

        def inverse(step, carry):
            rows = pl.ds(pl.multiple_of(step * 8, 8), 8)
            values = [(work_ref[k, 0, rows, :], work_ref[k, 1, rows, :]) for k in range(LOW)]
            for j, (real, imaginary) in enumerate(butterfly(values, 1.0)):
                buf[t, j, 0, rows, :] = real
                buf[t, j, 1, rows, :] = imaginary
            return carry

        lax.fori_loop(0, PART // 8, inverse, 0)

    def merge(t, q, other, at):
        def body(j, carry):
            buf[t, q * block + j] += other[t, at, j]
            return carry

        lax.fori_loop(0, block, body, 0)

    for t in range(min(AHEAD, total)):
        start_forward(t)

    def step(t, carry):
        @pl.when(t + AHEAD < total)
        def _():
            start_forward(t + AHEAD)

        @pl.when(t < total)
        def _():
            own_copy(t).wait()
            others(t, recv_f).wait()
            columns(t)

        right = t - here

        @pl.when(jnp.logical_and(right >= 0, right < total))
        def _():
            for q in range(depths - 1, 0, -1):
                @pl.when(jnp.logical_and(here > 0, q >= here))
                def _():
                    right_copy(right, q).wait_recv()
                    merge(right, q, rbuf, q - 1)

                @pl.when(q > here)
                def _():
                    right_copy(right, q).start()

        left = t - last

        @pl.when(jnp.logical_and(left >= 0, left < total))
        def _():
            for q in range(depths - 1):
                @pl.when(jnp.logical_and(last > 0, q <= here))
                def _():
                    left_copy(left, q).wait_recv()
                    merge(left, q, lbuf, q)

                @pl.when(q < here)
                def _():
                    left_copy(left, q).start()

        done = t - jnp.maximum(here, last)

        @pl.when(jnp.logical_and(done >= 0, done < total))
        def _():
            final_own(done).start()
            for step in range(1, owners):
                final_copy(done, (me + step) % owners).start()

        return carry

    lax.fori_loop(0, total + depths - 1, step, 0)

    def finish(t, carry):
        others(t, send_f).wait()
        for q in range(1, depths):
            @pl.when(q > here)
            def _():
                right_copy(t, q).wait_send()
        for q in range(depths - 1):
            @pl.when(q < here)
            def _():
                left_copy(t, q).wait_send()
        final_own(t).wait()
        finals(t, send_b).wait()
        finals(t, recv_b).wait()
        return carry

    lax.fori_loop(0, total, finish, 0)


def line(sent, scalars, tables, chunks, owners, depths):
    total = chunks * PARTS
    block = LOW // depths
    vmem = pl.BlockSpec(memory_space=pltpu.VMEM)
    hbm = pl.BlockSpec(memory_space=pl.ANY)
    dma = pltpu.SemaphoreType.DMA
    tile = (2, PART, HIGH)
    return pl.pallas_call(
        functools.partial(line_kernel, chunks, owners, depths),
        in_specs=[pl.BlockSpec(memory_space=pltpu.SMEM)] + [vmem] * len(tables) + [hbm],
        out_specs=hbm,
        out_shape=jax.ShapeDtypeStruct((total, owners) + tile, jnp.float32),
        scratch_shapes=[
            pltpu.VMEM((total, LOW) + tile, jnp.float32),
            pltpu.VMEM((total, depths - 1, block) + tile, jnp.float32),
            pltpu.VMEM((total, depths - 1, block) + tile, jnp.float32),
            pltpu.VMEM((LOW,) + tile, jnp.float32),
            dma((total,)), dma((total,)), dma((total,)),
            dma((total, depths - 1)), dma((total, depths - 1)),
            dma((total, depths - 1)), dma((total, depths - 1)),
            dma((total,)), dma((total,)), dma((total,)),
        ],
        compiler_params=pltpu.CompilerParams(vmem_limit_bytes=VMEM_LIMIT, collective_id=0, has_side_effects=True),
        name="line",
    )(scalars, *tables, sent)


def gather_kernel(chunks, in_ref, tr_ref, ti_ref, th_ref, tl_ref, o_ref, work_ref):
    def dense(k, carry):
        owner, chunk = k // chunks, k % chunks
        sides = [
            jnp.concatenate([in_ref[chunk * PARTS + part, owner, side] for part in range(PARTS)], axis=0).T for side in range(2)
        ]
        high, low = split(jnp.concatenate(sides, axis=1))
        out = dot(high, th_ref[...]) + dot(low, th_ref[...]) + dot(high, tl_ref[...])
        real, imaginary = out[:, :HIGH], out[:, HIGH:]
        turn_real, turn_imaginary = tr_ref[pl.ds(k, 1), :], ti_ref[pl.ds(k, 1), :]
        work_ref[k, 0] = real * turn_real - imaginary * turn_imaginary
        work_ref[k, 1] = real * turn_imaginary + imaginary * turn_real
        return carry

    lax.fori_loop(0, LOW, dense, 0, unroll=4)

    def body(step, carry):
        rows = pl.ds(pl.multiple_of(step * 8, 8), 8)
        values = [(work_ref[k, 0, rows, :], work_ref[k, 1, rows, :]) for k in range(LOW)]
        for j, (real, imaginary) in enumerate(butterfly(values, 1.0)):
            o_ref[0, rows, j * HIGH:(j + 1) * HIGH] = real
            o_ref[1, rows, j * HIGH:(j + 1) * HIGH] = imaginary
        return carry

    lax.fori_loop(0, HIGH // 8, body, 0)


def gather_width(parts, chunks, tables):
    vmem = pl.BlockSpec(memory_space=pltpu.VMEM)
    return pl.pallas_call(
        functools.partial(gather_kernel, chunks),
        in_specs=[vmem] * (1 + len(tables)),
        out_specs=vmem,
        out_shape=jax.ShapeDtypeStruct((2, HIGH, N), jnp.float32),
        scratch_shapes=[pltpu.VMEM((LOW, 2, HIGH, HIGH), jnp.float32)],
        compiler_params=pltpu.CompilerParams(vmem_limit_bytes=VMEM_LIMIT),
        name="gather",
    )(parts, *tables)


def fused(target, depth_index, band_mask):
    owners, depths = lax.axis_size("rows"), lax.axis_size("depth")
    chunks = LOW // owners
    field = target.reshape(target.shape[1:])
    scale = 1.0 / math.sqrt(N)
    forward, backward = dense_table(-1.0), dense_table(1.0)
    order = both(slots())
    turn = twiddles(-1.0, scale)
    turn_back = twiddles(1.0, scale / math.sqrt(depths))
    limits = (jnp.sum(band_mask[0], axis=-1) + 1) // 2
    scalars = jnp.stack([depth_index[0], limits[0], limits[1]]).astype(jnp.int32)
    sent = spread_width(field, chunks, owners, turn + halves(forward[order]))
    parts = line(sent, scalars, turn + halves(forward.T) + halves(backward.T), chunks, owners, depths)
    return gather_width(parts, chunks, turn_back + halves(backward.T[order]))


def solution(mesh):
    in_specs = (P("depth", None, "rows", None), P("depth"), P("depth", None, None))
    out_specs = P(None, ("depth", "rows"), None)
    step = jax.shard_map(local, mesh=mesh, in_specs=in_specs, out_specs=out_specs, check_vma=False)
    if mesh.shape["rows"] * mesh.shape["depth"] == LOW and mesh.shape["depth"] > 1:
        return jax.shard_map(fused, mesh=mesh, in_specs=in_specs, out_specs=out_specs, check_vma=False)
    return step
```

```python
import functools
import math

import jax
import jax.numpy as jnp
import numpy as np
from jax import lax
from jax.experimental import pallas as pl
from jax.experimental.pallas import tpu as pltpu
from jax.sharding import PartitionSpec as P


LOW = 32
HIGH = 128
N = LOW * HIGH
VMEM_LIMIT = 56 * 1024 * 1024


def scaled(value, factor_real, factor_imaginary):
    real, imaginary = value
    if abs(factor_imaginary) < 1e-12:
        if factor_real > 0:
            return (real, imaginary)
        return (-real, -imaginary)
    if abs(factor_real) < 1e-12:
        if factor_imaginary > 0:
            return (-imaginary, real)
        return (imaginary, -real)
    a, b = np.float32(factor_real), np.float32(factor_imaginary)
    return (real * a - imaginary * b, real * b + imaginary * a)


def root(numerator, length, direction):
    angle = direction * 2.0 * math.pi * (numerator % length) / length
    return math.cos(angle), math.sin(angle)


def add(left, right):
    return (left[0] + right[0], left[1] + right[1])


def subtract(left, right):
    return (left[0] - right[0], left[1] - right[1])


def butterfly(values, direction):
    count = len(values)
    if count == 1:
        return values
    even = butterfly(values[0::2], direction)
    odd = butterfly(values[1::2], direction)
    odd = [scaled(v, *root(k, count, direction)) for k, v in enumerate(odd)]
    return [add(e, o) for e, o in zip(even, odd)] + [subtract(e, o) for e, o in zip(even, odd)]


def dense_table(direction):
    index = np.arange(HIGH)
    angles = direction * 2.0 * np.pi / HIGH * (index[:, None] * index[None, :] % HIGH)
    cosine, sine = np.cos(angles), np.sin(angles)
    return np.block([[cosine, -sine], [sine, cosine]])


def halves(table):
    high = table.astype(np.float32).astype(jnp.bfloat16)
    low = (table - high.astype(np.float64)).astype(np.float32).astype(jnp.bfloat16)
    return jnp.asarray(high), jnp.asarray(low)


def twiddles(direction, scaling):
    product = np.arange(LOW)[:, None] * np.arange(HIGH)[None, :] % N
    angles = direction * 2.0 * np.pi / N * product
    return (
        jnp.asarray((np.cos(angles) * scaling).astype(np.float32)),
        jnp.asarray((np.sin(angles) * scaling).astype(np.float32)),
    )


def split(value):
    high = value.astype(jnp.bfloat16)
    return high, (value - high.astype(jnp.float32)).astype(jnp.bfloat16)


def tripled(value):
    high, low = split(value)
    return jnp.concatenate([high, low, high], axis=0)


def dot(left, right):
    return jnp.dot(left, right, preferred_element_type=jnp.float32)


def width_kernel(chunk, chunks, owners, x_ref, tr_ref, ti_ref, th_ref, tl_ref, o_ref, hi_ref, lo_ref):
    tile = x_ref.shape[1]

    def body(step, carry):
        rows = pl.ds(pl.multiple_of(step * 16, 16), 16)
        values = []
        for first in range(owners):
            total = None
            for second in range(chunks):
                at = (first + owners * second) * HIGH
                value = (x_ref[0, rows, at:at + HIGH], x_ref[1, rows, at:at + HIGH])
                value = scaled(value, *root(chunk * second, chunks, -1.0))
                total = value if total is None else add(total, value)
            values.append(scaled(total, *root(chunk * first, LOW, -1.0)))
        for owner, (real, imaginary) in enumerate(butterfly(values, -1.0)):
            k = chunks * owner + chunk
            turn_real, turn_imaginary = tr_ref[k:k + 1, :], ti_ref[k:k + 1, :]
            high, low = split(real * turn_real - imaginary * turn_imaginary)
            hi_ref[owner, rows, :HIGH] = high
            lo_ref[owner, rows, :HIGH] = low
            high, low = split(real * turn_imaginary + imaginary * turn_real)
            hi_ref[owner, rows, HIGH:] = high
            lo_ref[owner, rows, HIGH:] = low
        return carry

    lax.fori_loop(0, tile // 16, body, 0)
    for owner in range(owners):
        high = hi_ref[owner]
        out = dot(high, th_ref[...]) + dot(lo_ref[owner], th_ref[...]) + dot(high, tl_ref[...])
        o_ref[owner, 0] = out[:, :HIGH]
        o_ref[owner, 1] = out[:, HIGH:]


def along_width(field, chunk, chunks, owners, tables):
    _, height, _ = field.shape
    tile = min(128, height)
    whole = lambda a: pl.BlockSpec(a.shape, lambda i: (0,) * a.ndim)
    return pl.pallas_call(
        functools.partial(width_kernel, chunk, chunks, owners),
        grid=(height // tile,),
        in_specs=[pl.BlockSpec((2, tile, N), lambda i: (0, i, 0))] + [whole(a) for a in tables],
        out_specs=pl.BlockSpec((owners, 2, tile, HIGH), lambda i: (0, 0, i, 0)),
        out_shape=jax.ShapeDtypeStruct((owners, 2, height, HIGH), jnp.float32),
        scratch_shapes=[pltpu.VMEM((owners, tile, 2 * HIGH), jnp.bfloat16)] * 2,
        compiler_params=pltpu.CompilerParams(vmem_limit_bytes=VMEM_LIMIT),
        cost_estimate=pl.CostEstimate(flops=6 * height * HIGH * HIGH * 4 * owners * 2, bytes_accessed=field.size * 4 + field.size * 4 // chunks, transcendentals=0),
    )(field, *tables)


def series(values, points):
    nodes = np.cos(np.pi * (np.arange(400) + 0.5) / 400) * 0.125 + 0.125
    basis = np.polynomial.chebyshev.Chebyshev.fit(nodes, values(np.sqrt(nodes)), points, domain=[0.0, 0.25])
    return [np.float32(c) for c in basis.convert(kind=np.polynomial.Polynomial).coef]


COSINE = series(lambda r: np.cos(2.0 * np.pi * r), 6)
SINE = series(lambda r: np.sin(2.0 * np.pi * r) / r, 6)


def horner(coefficients, at):
    total = coefficients[-1]
    for c in coefficients[-2::-1]:
        total = total * at + c
    return total


def signed(natural):
    return jnp.where(natural < N // 2, natural, natural - N).astype(jnp.float32)


def column_kernel(scalars_ref, x_ref, tr_ref, ti_ref, f_ref, i_ref, o_ref, work_ref):
    owners, _, pieces, _, _ = x_ref.shape
    distance = scalars_ref[0].astype(jnp.float32) * 2.0 + 100.0
    limit_height = scalars_ref[1].astype(jnp.float32)
    limit_width = scalars_ref[2].astype(jnp.float32)
    column = scalars_ref[3]

    def forward(step, carry):
        rows = pl.ds(pl.multiple_of(step * 8, 8), 8)
        low_rows = pl.ds(pl.multiple_of(step * 8 + HIGH, 8), 8)
        values = [(x_ref[s, 0, p, rows, :], x_ref[s, 1, p, rows, :]) for s in range(owners) for p in range(pieces)]
        for k, (real, imaginary) in enumerate(butterfly(values, -1.0)):
            work_ref[k, rows, :] = real
            work_ref[k, low_rows, :] = imaginary
        return carry

    lax.fori_loop(0, HIGH // 8, forward, 0)

    across = signed(lax.broadcasted_iota(jnp.int32, (1, HIGH), 1) * LOW + column)
    inside_width = jnp.abs(across) < limit_width
    across_square = (across * (1.0 / N)) ** 2

    def turned(k):
        real, imaginary = work_ref[k, :HIGH, :], work_ref[k, HIGH:, :]
        turn_real, turn_imaginary = tr_ref[k], ti_ref[k]
        return jnp.concatenate(
            [real * turn_real - imaginary * turn_imaginary, real * turn_imaginary + imaginary * turn_real], axis=0
        )

    def propagate(k, real, imaginary):
        down = signed(lax.broadcasted_iota(jnp.int32, (HIGH, HIGH), 0) * LOW + k)
        square = (down * (1.0 / N)) ** 2 + across_square
        rest_square = 4.0 - square
        drop = 2.0 - rest_square * lax.rsqrt(rest_square)
        turns = -distance * (0.25 * (square + drop * drop))
        rest = turns - jnp.floor(turns + 0.5)
        at = rest * rest
        keep = jnp.logical_and(jnp.abs(down) < limit_height, inside_width)
        cosine = jnp.where(keep, horner(COSINE, at), 0.0)
        sine = jnp.where(keep, horner(SINE, at) * rest, 0.0)
        return jnp.concatenate([real * cosine - imaginary * sine, real * sine + imaginary * cosine], axis=0)

    def middle(step, carry):
        pair = [2 * step, 2 * step + 1]
        spectrum = dot(f_ref[...], tripled(jnp.concatenate([turned(k) for k in pair], axis=1)))
        moved = [
            propagate(k, spectrum[:HIGH, i * HIGH:(i + 1) * HIGH], spectrum[HIGH:, i * HIGH:(i + 1) * HIGH])
            for i, k in enumerate(pair)
        ]
        back = dot(i_ref[...], tripled(jnp.concatenate(moved, axis=1)))
        for i, k in enumerate(pair):
            real, imaginary = back[:HIGH, i * HIGH:(i + 1) * HIGH], back[HIGH:, i * HIGH:(i + 1) * HIGH]
            turn_real, turn_imaginary = tr_ref[k], ti_ref[k]
            work_ref[k, :HIGH, :] = real * turn_real + imaginary * turn_imaginary
            work_ref[k, HIGH:, :] = imaginary * turn_real - real * turn_imaginary
        return carry

    lax.fori_loop(0, LOW // 2, middle, 0)

    def inverse(step, carry):
        rows = pl.ds(pl.multiple_of(step * 8, 8), 8)
        low_rows = pl.ds(pl.multiple_of(step * 8 + HIGH, 8), 8)
        values = [(work_ref[k, rows, :], work_ref[k, low_rows, :]) for k in range(LOW)]
        for j, (real, imaginary) in enumerate(butterfly(values, 1.0)):
            o_ref[j, 0, rows, :] = real
            o_ref[j, 1, rows, :] = imaginary
        return carry

    lax.fori_loop(0, HIGH // 8, inverse, 0)


def columns_step(received, scalars, tables):
    owners, _, height, _ = received.shape
    received = received.reshape(owners, 2, height // HIGH, HIGH, HIGH)
    vmem = pl.BlockSpec(memory_space=pltpu.VMEM)
    return pl.pallas_call(
        column_kernel,
        in_specs=[pl.BlockSpec(memory_space=pltpu.SMEM)] + [vmem] * (1 + len(tables)),
        out_specs=vmem,
        out_shape=jax.ShapeDtypeStruct((LOW, 2, HIGH, HIGH), jnp.float32),
        scratch_shapes=[pltpu.VMEM((LOW, 2 * HIGH, HIGH), jnp.float32)],
        compiler_params=pltpu.CompilerParams(vmem_limit_bytes=VMEM_LIMIT),
        cost_estimate=pl.CostEstimate(flops=12 * LOW * HIGH * 256 * 256 * 2, bytes_accessed=16 * 1024 * 1024, transcendentals=0),
    )(scalars, received, *tables)


def output_kernel(chunks, *refs):
    inputs = refs[:chunks]
    tr_ref, ti_ref, th_ref, tl_ref, o_ref, work_ref = refs[chunks:]
    owners, _, height, _ = inputs[0].shape
    for owner in range(owners):
        for chunk in range(chunks):
            k = chunks * owner + chunk
            value = jnp.concatenate([inputs[chunk][owner, 0], inputs[chunk][owner, 1]], axis=1)
            high, low = split(value)
            out = dot(high, th_ref[...]) + dot(low, th_ref[...]) + dot(high, tl_ref[...])
            real, imaginary = out[:, :HIGH], out[:, HIGH:]
            turn_real, turn_imaginary = tr_ref[k:k + 1, :], ti_ref[k:k + 1, :]
            work_ref[k, 0] = real * turn_real - imaginary * turn_imaginary
            work_ref[k, 1] = real * turn_imaginary + imaginary * turn_real

    def body(step, carry):
        rows = pl.ds(pl.multiple_of(step * 8, 8), 8)
        values = [(work_ref[k, 0, rows, :], work_ref[k, 1, rows, :]) for k in range(LOW)]
        for j, (real, imaginary) in enumerate(butterfly(values, 1.0)):
            o_ref[0, rows, j * HIGH:(j + 1) * HIGH] = real
            o_ref[1, rows, j * HIGH:(j + 1) * HIGH] = imaginary
        return carry

    lax.fori_loop(0, height // 8, body, 0)


def inverse_width(parts, tables):
    height = parts[0].shape[2]
    vmem = pl.BlockSpec(memory_space=pltpu.VMEM)
    return pl.pallas_call(
        functools.partial(output_kernel, len(parts)),
        in_specs=[vmem] * (len(parts) + len(tables)),
        out_specs=vmem,
        out_shape=jax.ShapeDtypeStruct((2, height, N), jnp.float32),
        scratch_shapes=[pltpu.VMEM((LOW, 2, height, HIGH), jnp.float32)],
        compiler_params=pltpu.CompilerParams(vmem_limit_bytes=VMEM_LIMIT),
        cost_estimate=pl.CostEstimate(flops=6 * LOW * height * 256 * 256, bytes_accessed=8 * height * N * 2, transcendentals=0),
        name="output",
    )(*parts, *tables)


def local(target, depth_index, band_mask):
    owners, depths = lax.axis_size("rows"), lax.axis_size("depth")
    chunks = LOW // owners
    field = target.reshape(target.shape[1:])
    scale = 1.0 / math.sqrt(N)
    forward, backward = dense_table(-1.0), dense_table(1.0)
    left = tuple(jnp.concatenate([h, h, l], axis=1) for h, l in (halves(forward), halves(backward)))
    forward_right, backward_right = halves(forward.T), halves(backward.T)
    turn = twiddles(-1.0, scale)
    turn_back = twiddles(1.0, scale / math.sqrt(depths))
    spread = tuple(jnp.broadcast_to(t[:, :, None], (LOW, HIGH, HIGH)) for t in turn)
    limits = (jnp.sum(band_mask[0], axis=-1) + 1) // 2
    me = lax.axis_index("rows")
    rows = N // (owners * depths)

    pieces = []
    for chunk in range(chunks):
        sent = along_width(field, chunk, chunks, owners, turn + forward_right)
        received = lax.all_to_all(sent, "rows", split_axis=0, concat_axis=0, tiled=True)
        scalars = jnp.stack([depth_index[0], limits[0], limits[1], me * chunks + chunk]).astype(jnp.int32)
        part = columns_step(received, scalars, spread + left)
        pieces.append(lax.psum_scatter(part, "depth", scatter_dimension=0, tiled=True))
    results = []
    for share in pieces:
        share = share.reshape(share.shape[0], 2, HIGH // rows, rows, HIGH)
        share = jnp.transpose(share, (0, 2, 1, 3, 4)).reshape(owners, 2, rows, HIGH)
        results.append(lax.all_to_all(share, "rows", split_axis=0, concat_axis=0, tiled=True))
    return inverse_width(results, turn_back + backward_right)


MESH = pl.DeviceIdType.MESH
PART = 16
PARTS = HIGH // PART
LINE_VMEM = 62 * 1024 * 1024


def slots():
    half = PART // 2
    order = []
    for part in range(PARTS):
        order += list(range(half * part, half * (part + 1)))
        order += list(range(HIGH - half * (part + 1), HIGH - half * part))
    return np.array(order)


def both(index):
    return np.concatenate([index, index + HIGH])


def nt_dot(left, right):
    return lax.dot_general(left, right, (((1,), (1,)), ((), ())), preferred_element_type=jnp.float32)


def width_rows(chunk, chunks, owners, x_at, rows, target, tr_ref, ti_ref, v_ref):
    values = []
    for first in range(owners):
        total = None
        for second in range(chunks):
            at = (first + owners * second) * HIGH
            value = scaled((x_at(0, rows, at), x_at(1, rows, at)), *root(chunk * second, chunks, -1.0))
            total = value if total is None else add(total, value)
        values.append(scaled(total, *root(chunk * first, LOW, -1.0)))
    for owner, (real, imaginary) in enumerate(butterfly(values, -1.0)):
        k = chunks * owner + chunk
        turn_real, turn_imaginary = tr_ref[k:k + 1, :], ti_ref[k:k + 1, :]
        v_ref[owner, target, :HIGH] = real * turn_real - imaginary * turn_imaginary
        v_ref[owner, target, HIGH:] = real * turn_imaginary + imaginary * turn_real


def width_dense(step, th_ref, tl_ref, v_ref, put):
    value = jnp.concatenate([v_ref[2 * step], v_ref[2 * step + 1]], axis=0)
    high, low = split(value)
    out = nt_dot(th_ref[...], high) + nt_dot(th_ref[...], low) + nt_dot(tl_ref[...], high)
    for i in range(2):
        for part in range(PARTS):
            for side in range(2):
                at = side * HIGH + part * PART
                put(part, 2 * step + i, side, out[at:at + PART, i * HIGH:(i + 1) * HIGH])


def spread_kernel(chunks, owners, x_ref, tr_ref, ti_ref, th_ref, tl_ref, o_ref, v_ref):
    def body(step, carry):
        rows = pl.ds(pl.multiple_of(step * 8, 8), 8)
        width_rows(0, chunks, owners, lambda side, r, at: x_ref[side, r, at:at + HIGH], rows, rows, tr_ref, ti_ref, v_ref)
        return carry

    lax.fori_loop(0, HIGH // 8, body, 0)

    def put(part, owner, side, value):
        o_ref[part, owner, 0, side] = value

    def dense(step, carry):
        width_dense(step, th_ref, tl_ref, v_ref, put)
        return carry

    lax.fori_loop(0, owners // 2, dense, 0)


def spread_width(field, chunks, owners, tables):
    _, height, _ = field.shape
    whole = lambda a: pl.BlockSpec(a.shape, lambda i: (0,) * a.ndim)
    shape = (PARTS, owners, height // HIGH, 2, PART, HIGH)
    return pl.pallas_call(
        functools.partial(spread_kernel, chunks, owners),
        grid=(height // HIGH,),
        in_specs=[pl.BlockSpec((2, HIGH, N), lambda i: (0, i, 0))] + [whole(a) for a in tables],
        out_specs=pl.BlockSpec(shape[:2] + (1,) + shape[3:], lambda i: (0, 0, i, 0, 0, 0)),
        out_shape=jax.ShapeDtypeStruct(shape, jnp.float32),
        scratch_shapes=[pltpu.VMEM((owners, HIGH, 2 * HIGH), jnp.float32)],
        compiler_params=pltpu.CompilerParams(vmem_limit_bytes=VMEM_LIMIT),
        name="spread",
    )(field, *tables)


def line_kernel(chunks, owners, depths, outer, levels, scalars_ref, tr_ref, ti_ref, th_ref, tl_ref, fh_ref, fl_ref, ih_ref, il_ref,
                sent_ref, x_ref, back_ref, buf, zbuf, stage, xbuf, v_ref, work_ref,
                self_f, send_f, recv_f, send_r, recv_r, send_l, recv_l, self_b, send_b, recv_b, x_sem):
    total = chunks * levels
    block = LOW // depths
    pieces = LOW // owners
    ahead = max(1, levels - pieces)
    halves_all = (chunks - 1) * pieces * 2
    tall = HIGH // 2
    here, me = lax.axis_index("depth"), lax.axis_index("rows")
    last = depths - 1 - here
    inner = jnp.minimum(here, 1) * jnp.minimum(last, 1)
    mine = outer + (levels - outer) * inner

    def active(t):
        return t % levels < mine

    def filled(t):
        return t % levels < outer

    def when(*conditions):
        return pl.when(functools.reduce(jnp.logical_and, conditions))

    def x_copy(h):
        return pltpu.make_async_copy(x_ref.at[:, pl.ds((h % (2 * pieces)) * tall, tall), :], xbuf.at[h % 2], x_sem.at[h % 2])

    for h in range(min(2, halves_all)):
        x_copy(h).start()

    barrier = pltpu.get_barrier_semaphore()
    for step in range(1, owners):
        pl.semaphore_signal(barrier, inc=1, device_id=(here, (me + step) % owners), device_id_type=MESH)

    @pl.when(here > 0)
    def _():
        pl.semaphore_signal(barrier, inc=1, device_id=(here - 1, me), device_id_type=MESH)

    @pl.when(last > 0)
    def _():
        pl.semaphore_signal(barrier, inc=1, device_id=(here + 1, me), device_id_type=MESH)

    pl.semaphore_wait(barrier, owners - 1 + jnp.minimum(here, 1) + jnp.minimum(last, 1))

    def forward_copies(source, t):
        pltpu.make_async_copy(source.at[me], buf.at[t, pl.ds(me * pieces, pieces)], self_f.at[t]).start()
        for step in range(1, owners):
            peer = (me + step) % owners
            pltpu.make_async_remote_copy(
                src_ref=source.at[peer],
                dst_ref=buf.at[t, pl.ds(me * pieces, pieces)],
                send_sem=send_f.at[t],
                recv_sem=recv_f.at[t],
                device_id=(here, peer),
                device_id_type=MESH,
            ).start()

    def start_forward(t):
        group, part = t // levels, t % levels

        @when(active(t), group == 0)
        def _():
            forward_copies(sent_ref.at[part], t)

        @when(active(t), group > 0)
        def _():
            forward_copies(stage.at[(group + 1) % 2, part], t)

    def arrived(t):
        some = buf.at[t, pl.ds(me * pieces, pieces)]
        return pltpu.make_async_copy(some, some, self_f.at[t])

    def others(t, sem):
        some = buf.at[t, pl.ds(0, pieces * (owners - 1))]
        return pltpu.make_async_copy(some, some, sem.at[t])

    def right_copy(t, q):
        return pltpu.make_async_remote_copy(
            src_ref=buf.at[t, pl.ds(q * block, block)],
            dst_ref=zbuf.at[t, q - here - 1],
            send_sem=send_r.at[t, q - 1],
            recv_sem=recv_r.at[t, q - 1],
            device_id=(here + 1, me),
            device_id_type=MESH,
        )

    def left_copy(t, q):
        return pltpu.make_async_remote_copy(
            src_ref=buf.at[t, pl.ds(q * block, block)],
            dst_ref=zbuf.at[t, depths - here + 1 + q],
            send_sem=send_l.at[t, q],
            recv_sem=recv_l.at[t, q],
            device_id=(here - 1, me),
            device_id_type=MESH,
        )

    def landed(t, at, sem):
        some = zbuf.at[t, at]
        return pltpu.make_async_copy(some, some, sem)

    def final_place(t):
        return back_ref.at[(t // levels) * PARTS + t % levels]

    def final_copy(t, peer):
        return pltpu.make_async_remote_copy(
            src_ref=buf.at[t, here * block + peer],
            dst_ref=final_place(t).at[me],
            send_sem=send_b.at[t],
            recv_sem=recv_b.at[t],
            device_id=(here, peer),
            device_id_type=MESH,
        )

    def final_own(t):
        return pltpu.make_async_copy(buf.at[t, here * block + me], final_place(t).at[me], self_b.at[t])

    def finals(t, sem):
        some = final_place(t).at[pl.ds(0, owners - 1)]
        return pltpu.make_async_copy(some, some, sem.at[t])

    distance = scalars_ref[0].astype(jnp.float32) * 2.0 + 100.0
    limit_height = scalars_ref[1].astype(jnp.float32)
    limit_width = scalars_ref[2].astype(jnp.float32)

    def columns(t):
        def forward(step, carry):
            rows = pl.ds(pl.multiple_of(step * 8, 8), 8)
            values = [(buf[t, p, 0, rows, :], buf[t, p, 1, rows, :]) for p in range(LOW)]
            for k, (real, imaginary) in enumerate(butterfly(values, -1.0)):
                work_ref[k, 0, rows, :] = real
                work_ref[k, 1, rows, :] = imaginary
            return carry

        lax.fori_loop(0, PART // 8, forward, 0)

        column = me * chunks + t // levels
        part = t % levels
        half = PART // 2
        slot = lax.broadcasted_iota(jnp.int32, (PART, HIGH), 0)
        turn = jnp.where(slot < half, half * part + slot, slot - half - half * (part + 1))
        across = (column + LOW * turn).astype(jnp.float32)
        inside_width = jnp.abs(across) < limit_width
        across_square = (across * (1.0 / N)) ** 2
        lanes = lax.broadcasted_iota(jnp.int32, (1, HIGH), 1) * LOW
        group = 16

        def middle(step, carry):
            taken = []
            for i in range(group):
                k = group * step + i
                real, imaginary = work_ref[k, 0], work_ref[k, 1]
                turn_real, turn_imaginary = tr_ref[pl.ds(k, 1), :], ti_ref[pl.ds(k, 1), :]
                taken.append(jnp.concatenate(
                    [real * turn_real - imaginary * turn_imaginary, real * turn_imaginary + imaginary * turn_real], axis=1))
            high, low = split(jnp.concatenate(taken, axis=0))
            spectrum = dot(high, fh_ref[...]) + dot(low, fh_ref[...]) + dot(high, fl_ref[...])
            moved = []
            for i in range(group):
                real, imaginary = spectrum[i * PART:(i + 1) * PART, :HIGH], spectrum[i * PART:(i + 1) * PART, HIGH:]
                down = signed(lanes + (group * step + i))
                square = (down * (1.0 / N)) ** 2 + across_square
                rest_square = 4.0 - square
                drop = 2.0 - rest_square * lax.rsqrt(rest_square)
                turns = -distance * (0.25 * (square + drop * drop))
                rest = turns - jnp.floor(turns + 0.5)
                at = rest * rest
                keep = jnp.logical_and(jnp.abs(down) < limit_height, inside_width)
                cosine = jnp.where(keep, horner(COSINE, at), 0.0)
                sine = jnp.where(keep, horner(SINE, at) * rest, 0.0)
                moved.append(jnp.concatenate([real * cosine - imaginary * sine, real * sine + imaginary * cosine], axis=1))
            high, low = split(jnp.concatenate(moved, axis=0))
            back = dot(high, ih_ref[...]) + dot(low, ih_ref[...]) + dot(high, il_ref[...])
            for i in range(group):
                k = group * step + i
                real, imaginary = back[i * PART:(i + 1) * PART, :HIGH], back[i * PART:(i + 1) * PART, HIGH:]
                turn_real, turn_imaginary = tr_ref[pl.ds(k, 1), :], ti_ref[pl.ds(k, 1), :]
                work_ref[k, 0] = real * turn_real + imaginary * turn_imaginary
                work_ref[k, 1] = imaginary * turn_real - real * turn_imaginary
            return carry

        lax.fori_loop(0, LOW // group, middle, 0)

        def inverse(step, carry):
            rows = pl.ds(pl.multiple_of(step * 8, 8), 8)
            values = [(work_ref[k, 0, rows, :], work_ref[k, 1, rows, :]) for k in range(LOW)]
            for j, (real, imaginary) in enumerate(butterfly(values, 1.0)):
                buf[t, j, 0, rows, :] = real
                buf[t, j, 1, rows, :] = imaginary
            return carry

        lax.fori_loop(0, PART // 8, inverse, 0)

    def merge(t, q, at):
        @pl.when(active(t))
        def _():
            def body(j, carry):
                buf[t, q * block + j] += zbuf[t, at, j]
                return carry

            lax.fori_loop(0, block, body, 0)

        if outer < levels:
            @pl.when(jnp.logical_not(active(t)))
            def _():
                def body(j, carry):
                    buf[t, q * block + j] = zbuf[t, at, j]
                    return carry

                lax.fori_loop(0, block, body, 0)

    def width_tile(chunk, piece):
        for half in range(2):
            h = ((chunk - 1) * pieces + piece) * 2 + half
            x_copy(h).wait()

            def body(step, carry):
                rows = pl.ds(pl.multiple_of(step * 8, 8), 8)
                target = pl.ds(pl.multiple_of(step * 8 + half * tall, 8), 8)
                width_rows(chunk, chunks, owners, lambda side, r, at: xbuf[half, side, r, at:at + HIGH], rows, target, tr_ref, ti_ref, v_ref)
                return carry

            lax.fori_loop(0, tall // 8, body, 0)

            @pl.when(h + 2 < halves_all)
            def _():
                x_copy(h + 2).start()

        def put(part, owner, side, value):
            if isinstance(part, int) and part >= levels:
                return
            stage[(chunk + 1) % 2, part, owner, piece, side] = value

        def dense(step, carry):
            width_dense(step, th_ref, tl_ref, v_ref, put)
            return carry

        lax.fori_loop(0, owners // 2, dense, 0)

    def begin(t, carry):
        start_forward(t)
        return carry

    lax.fori_loop(0, min(ahead, total), begin, 0)

    def step(t, carry):
        @pl.when(t + ahead < total)
        def _():
            start_forward(t + ahead)

        @when(t < total, active(t))
        def _():
            arrived(t).wait()
            others(t, recv_f).wait()
            columns(t)

        right = t - here

        @when(right >= 0, right < total)
        def _():
            for q in range(depths - 1, 0, -1):
                @when(here > 0, q >= here, jnp.logical_or(here > 1, filled(right)))
                def _():
                    landed(right, q - here, recv_r.at[right, q - 1]).wait()
                    merge(right, q, q - here)

                @when(q > here, jnp.logical_or(here > 0, filled(right)))
                def _():
                    right_copy(right, q).start()

        left = t - last

        @when(left >= 0, left < total)
        def _():
            for q in range(depths - 1):
                @when(last > 0, q <= here, jnp.logical_or(last > 1, filled(left)))
                def _():
                    landed(left, depths - here + q, recv_l.at[left, q]).wait()
                    merge(left, q, depths - here + q)

                @when(q < here, jnp.logical_or(last > 0, filled(left)))
                def _():
                    left_copy(left, q).start()

        done = t - jnp.maximum(here, last)

        @when(done >= 0, done < total)
        def _():
            final_own(done).start()
            for step in range(1, owners):
                final_copy(done, (me + step) % owners).start()

        group, piece = t // levels, t % levels
        for chunk in range(1, chunks):
            @when(group == chunk - 1, piece < pieces)
            def _():
                if chunk > 2:
                    @pl.when(piece == 0)
                    def _():
                        def free(part, carry):
                            @pl.when(active(part))
                            def _():
                                others((chunk - 2) * levels + part, send_f).wait()

                            return carry

                        lax.fori_loop(0, levels, free, 0)
                width_tile(chunk, piece)

        return carry

    lax.fori_loop(0, total + depths - 1, step, 0)

    def finish(t, carry):
        group = t // levels

        @when(active(t), jnp.logical_or(group == 0, group + 2 >= chunks))
        def _():
            others(t, send_f).wait()

        for q in range(1, depths):
            @when(q > here, jnp.logical_or(here > 0, filled(t)))
            def _():
                right_copy(t, q).wait_send()
        for q in range(depths - 1):
            @when(q < here, jnp.logical_or(last > 0, filled(t)))
            def _():
                left_copy(t, q).wait_send()
        final_own(t).wait()
        finals(t, send_b).wait()
        finals(t, recv_b).wait()
        return carry

    lax.fori_loop(0, total, finish, 0)


def line(sent, field, scalars, tables, chunks, owners, depths, outer, levels):
    total = chunks * levels
    block = LOW // depths
    pieces = LOW // owners
    vmem = pl.BlockSpec(memory_space=pltpu.VMEM)
    hbm = pl.BlockSpec(memory_space=pl.ANY)
    dma = pltpu.SemaphoreType.DMA
    tile = (2, PART, HIGH)
    return pl.pallas_call(
        functools.partial(line_kernel, chunks, owners, depths, outer, levels),
        in_specs=[pl.BlockSpec(memory_space=pltpu.SMEM)] + [vmem] * len(tables) + [hbm, hbm],
        out_specs=hbm,
        out_shape=jax.ShapeDtypeStruct((chunks * PARTS, owners) + tile, jnp.float32),
        scratch_shapes=[
            pltpu.VMEM((total, LOW) + tile, jnp.float32),
            pltpu.VMEM((total, depths + 1, block) + tile, jnp.float32),
            pltpu.VMEM((2, levels, owners, pieces) + tile, jnp.float32),
            pltpu.VMEM((2, 2, HIGH // 2, N), jnp.float32),
            pltpu.VMEM((owners, HIGH, 2 * HIGH), jnp.float32),
            pltpu.VMEM((LOW,) + tile, jnp.float32),
            dma((total,)), dma((total,)), dma((total,)),
            dma((total, depths - 1)), dma((total, depths - 1)),
            dma((total, depths - 1)), dma((total, depths - 1)),
            dma((total,)), dma((total,)), dma((total,)),
            dma((2,)),
        ],
        compiler_params=pltpu.CompilerParams(vmem_limit_bytes=LINE_VMEM, collective_id=0, has_side_effects=True),
        name="line",
    )(scalars, *tables, sent, field)


def gather_kernel(chunks, in_ref, tr_ref, ti_ref, th_ref, tl_ref, o_ref, work_ref):
    def dense(k, carry):
        owner, chunk = k // chunks, k % chunks
        sides = [
            jnp.concatenate([in_ref[chunk * PARTS + part, owner, side] for part in range(PARTS)], axis=0).T for side in range(2)
        ]
        high, low = split(jnp.concatenate(sides, axis=1))
        out = dot(high, th_ref[...]) + dot(low, th_ref[...]) + dot(high, tl_ref[...])
        real, imaginary = out[:, :HIGH], out[:, HIGH:]
        turn_real, turn_imaginary = tr_ref[pl.ds(k, 1), :], ti_ref[pl.ds(k, 1), :]
        work_ref[k, 0] = real * turn_real - imaginary * turn_imaginary
        work_ref[k, 1] = real * turn_imaginary + imaginary * turn_real
        return carry

    lax.fori_loop(0, LOW, dense, 0, unroll=4)

    def body(step, carry):
        rows = pl.ds(pl.multiple_of(step * 8, 8), 8)
        values = [(work_ref[k, 0, rows, :], work_ref[k, 1, rows, :]) for k in range(LOW)]
        for j, (real, imaginary) in enumerate(butterfly(values, 1.0)):
            o_ref[0, rows, j * HIGH:(j + 1) * HIGH] = real
            o_ref[1, rows, j * HIGH:(j + 1) * HIGH] = imaginary
        return carry

    lax.fori_loop(0, HIGH // 8, body, 0)


def gather_width(parts, chunks, tables):
    vmem = pl.BlockSpec(memory_space=pltpu.VMEM)
    return pl.pallas_call(
        functools.partial(gather_kernel, chunks),
        in_specs=[vmem] * (1 + len(tables)),
        out_specs=vmem,
        out_shape=jax.ShapeDtypeStruct((2, HIGH, N), jnp.float32),
        scratch_shapes=[pltpu.VMEM((LOW, 2, HIGH, HIGH), jnp.float32)],
        compiler_params=pltpu.CompilerParams(vmem_limit_bytes=VMEM_LIMIT),
        name="gather",
    )(parts, *tables)


def fused(target, depth_index, band_mask):
    owners, depths = lax.axis_size("rows"), lax.axis_size("depth")
    chunks = LOW // owners
    field = target.reshape(target.shape[1:])
    scale = 1.0 / math.sqrt(N)
    forward, backward = dense_table(-1.0), dense_table(1.0)
    order = both(slots())
    turn = twiddles(-1.0, scale)
    turn_back = twiddles(1.0, scale / math.sqrt(depths))
    limits = (jnp.sum(band_mask[0], axis=-1) + 1) // 2
    scalars = jnp.stack([depth_index[0], limits[0], limits[1]]).astype(jnp.int32)
    wide = halves(forward[order])
    sent = spread_width(field, chunks, owners, turn + wide)
    tables = turn + wide + halves(forward.T) + halves(backward.T)
    parts = line(sent, field, scalars, tables, chunks, owners, depths, PARTS, PARTS)
    return gather_width(parts, chunks, turn_back + halves(backward.T[order]))


def solution(mesh):
    in_specs = (P("depth", None, "rows", None), P("depth"), P("depth", None, None))
    out_specs = P(None, ("depth", "rows"), None)
    step = jax.shard_map(local, mesh=mesh, in_specs=in_specs, out_specs=out_specs, check_vma=False)
    if mesh.shape["rows"] * mesh.shape["depth"] == LOW and mesh.shape["depth"] > 1:
        return jax.shard_map(fused, mesh=mesh, in_specs=in_specs, out_specs=out_specs, check_vma=False)
    return step
```

```python
import functools
import math

import jax
import jax.numpy as jnp
import numpy as np
from jax import lax
from jax.experimental import pallas as pl
from jax.experimental.pallas import tpu as pltpu
from jax.sharding import PartitionSpec as P


LOW = 32
HIGH = 128
N = LOW * HIGH
VMEM_LIMIT = 56 * 1024 * 1024


def scaled(value, factor_real, factor_imaginary):
    real, imaginary = value
    if abs(factor_imaginary) < 1e-12:
        if factor_real > 0:
            return (real, imaginary)
        return (-real, -imaginary)
    if abs(factor_real) < 1e-12:
        if factor_imaginary > 0:
            return (-imaginary, real)
        return (imaginary, -real)
    a, b = np.float32(factor_real), np.float32(factor_imaginary)
    return (real * a - imaginary * b, real * b + imaginary * a)


def root(numerator, length, direction):
    angle = direction * 2.0 * math.pi * (numerator % length) / length
    return math.cos(angle), math.sin(angle)


def add(left, right):
    return (left[0] + right[0], left[1] + right[1])


def subtract(left, right):
    return (left[0] - right[0], left[1] - right[1])


def butterfly(values, direction):
    count = len(values)
    if count == 1:
        return values
    even = butterfly(values[0::2], direction)
    odd = butterfly(values[1::2], direction)
    odd = [scaled(v, *root(k, count, direction)) for k, v in enumerate(odd)]
    return [add(e, o) for e, o in zip(even, odd)] + [subtract(e, o) for e, o in zip(even, odd)]


def dense_table(direction):
    index = np.arange(HIGH)
    angles = direction * 2.0 * np.pi / HIGH * (index[:, None] * index[None, :] % HIGH)
    cosine, sine = np.cos(angles), np.sin(angles)
    return np.block([[cosine, -sine], [sine, cosine]])


def halves(table):
    high = table.astype(np.float32).astype(jnp.bfloat16)
    low = (table - high.astype(np.float64)).astype(np.float32).astype(jnp.bfloat16)
    return jnp.asarray(high), jnp.asarray(low)


def twiddles(direction, scaling):
    product = np.arange(LOW)[:, None] * np.arange(HIGH)[None, :] % N
    angles = direction * 2.0 * np.pi / N * product
    return (
        jnp.asarray((np.cos(angles) * scaling).astype(np.float32)),
        jnp.asarray((np.sin(angles) * scaling).astype(np.float32)),
    )


def split(value):
    high = value.astype(jnp.bfloat16)
    return high, (value - high.astype(jnp.float32)).astype(jnp.bfloat16)


def tripled(value):
    high, low = split(value)
    return jnp.concatenate([high, low, high], axis=0)


def dot(left, right):
    return jnp.dot(left, right, preferred_element_type=jnp.float32)


def width_kernel(chunk, chunks, owners, x_ref, tr_ref, ti_ref, th_ref, tl_ref, o_ref, hi_ref, lo_ref):
    tile = x_ref.shape[1]

    def body(step, carry):
        rows = pl.ds(pl.multiple_of(step * 16, 16), 16)
        values = []
        for first in range(owners):
            total = None
            for second in range(chunks):
                at = (first + owners * second) * HIGH
                value = (x_ref[0, rows, at:at + HIGH], x_ref[1, rows, at:at + HIGH])
                value = scaled(value, *root(chunk * second, chunks, -1.0))
                total = value if total is None else add(total, value)
            values.append(scaled(total, *root(chunk * first, LOW, -1.0)))
        for owner, (real, imaginary) in enumerate(butterfly(values, -1.0)):
            k = chunks * owner + chunk
            turn_real, turn_imaginary = tr_ref[k:k + 1, :], ti_ref[k:k + 1, :]
            high, low = split(real * turn_real - imaginary * turn_imaginary)
            hi_ref[owner, rows, :HIGH] = high
            lo_ref[owner, rows, :HIGH] = low
            high, low = split(real * turn_imaginary + imaginary * turn_real)
            hi_ref[owner, rows, HIGH:] = high
            lo_ref[owner, rows, HIGH:] = low
        return carry

    lax.fori_loop(0, tile // 16, body, 0)
    for owner in range(owners):
        high = hi_ref[owner]
        out = dot(high, th_ref[...]) + dot(lo_ref[owner], th_ref[...]) + dot(high, tl_ref[...])
        o_ref[owner, 0] = out[:, :HIGH]
        o_ref[owner, 1] = out[:, HIGH:]


def along_width(field, chunk, chunks, owners, tables):
    _, height, _ = field.shape
    tile = min(128, height)
    whole = lambda a: pl.BlockSpec(a.shape, lambda i: (0,) * a.ndim)
    return pl.pallas_call(
        functools.partial(width_kernel, chunk, chunks, owners),
        grid=(height // tile,),
        in_specs=[pl.BlockSpec((2, tile, N), lambda i: (0, i, 0))] + [whole(a) for a in tables],
        out_specs=pl.BlockSpec((owners, 2, tile, HIGH), lambda i: (0, 0, i, 0)),
        out_shape=jax.ShapeDtypeStruct((owners, 2, height, HIGH), jnp.float32),
        scratch_shapes=[pltpu.VMEM((owners, tile, 2 * HIGH), jnp.bfloat16)] * 2,
        compiler_params=pltpu.CompilerParams(vmem_limit_bytes=VMEM_LIMIT),
        cost_estimate=pl.CostEstimate(flops=6 * height * HIGH * HIGH * 4 * owners * 2, bytes_accessed=field.size * 4 + field.size * 4 // chunks, transcendentals=0),
    )(field, *tables)


def series(values, points):
    nodes = np.cos(np.pi * (np.arange(400) + 0.5) / 400) * 0.125 + 0.125
    basis = np.polynomial.chebyshev.Chebyshev.fit(nodes, values(np.sqrt(nodes)), points, domain=[0.0, 0.25])
    return [np.float32(c) for c in basis.convert(kind=np.polynomial.Polynomial).coef]


COSINE = series(lambda r: np.cos(2.0 * np.pi * r), 6)
SINE = series(lambda r: np.sin(2.0 * np.pi * r) / r, 6)


def horner(coefficients, at):
    total = coefficients[-1]
    for c in coefficients[-2::-1]:
        total = total * at + c
    return total


def signed(natural):
    return jnp.where(natural < N // 2, natural, natural - N).astype(jnp.float32)


def column_kernel(scalars_ref, x_ref, tr_ref, ti_ref, f_ref, i_ref, o_ref, work_ref):
    owners, _, pieces, _, _ = x_ref.shape
    distance = scalars_ref[0].astype(jnp.float32) * 2.0 + 100.0
    limit_height = scalars_ref[1].astype(jnp.float32)
    limit_width = scalars_ref[2].astype(jnp.float32)
    column = scalars_ref[3]

    def forward(step, carry):
        rows = pl.ds(pl.multiple_of(step * 8, 8), 8)
        low_rows = pl.ds(pl.multiple_of(step * 8 + HIGH, 8), 8)
        values = [(x_ref[s, 0, p, rows, :], x_ref[s, 1, p, rows, :]) for s in range(owners) for p in range(pieces)]
        for k, (real, imaginary) in enumerate(butterfly(values, -1.0)):
            work_ref[k, rows, :] = real
            work_ref[k, low_rows, :] = imaginary
        return carry

    lax.fori_loop(0, HIGH // 8, forward, 0)

    across = signed(lax.broadcasted_iota(jnp.int32, (1, HIGH), 1) * LOW + column)
    inside_width = jnp.abs(across) < limit_width
    across_square = (across * (1.0 / N)) ** 2

    def turned(k):
        real, imaginary = work_ref[k, :HIGH, :], work_ref[k, HIGH:, :]
        turn_real, turn_imaginary = tr_ref[k], ti_ref[k]
        return jnp.concatenate(
            [real * turn_real - imaginary * turn_imaginary, real * turn_imaginary + imaginary * turn_real], axis=0
        )

    def propagate(k, real, imaginary):
        down = signed(lax.broadcasted_iota(jnp.int32, (HIGH, HIGH), 0) * LOW + k)
        square = (down * (1.0 / N)) ** 2 + across_square
        rest_square = 4.0 - square
        drop = 2.0 - rest_square * lax.rsqrt(rest_square)
        turns = -distance * (0.25 * (square + drop * drop))
        rest = turns - jnp.floor(turns + 0.5)
        at = rest * rest
        keep = jnp.logical_and(jnp.abs(down) < limit_height, inside_width)
        cosine = jnp.where(keep, horner(COSINE, at), 0.0)
        sine = jnp.where(keep, horner(SINE, at) * rest, 0.0)
        return jnp.concatenate([real * cosine - imaginary * sine, real * sine + imaginary * cosine], axis=0)

    def middle(step, carry):
        pair = [2 * step, 2 * step + 1]
        spectrum = dot(f_ref[...], tripled(jnp.concatenate([turned(k) for k in pair], axis=1)))
        moved = [
            propagate(k, spectrum[:HIGH, i * HIGH:(i + 1) * HIGH], spectrum[HIGH:, i * HIGH:(i + 1) * HIGH])
            for i, k in enumerate(pair)
        ]
        back = dot(i_ref[...], tripled(jnp.concatenate(moved, axis=1)))
        for i, k in enumerate(pair):
            real, imaginary = back[:HIGH, i * HIGH:(i + 1) * HIGH], back[HIGH:, i * HIGH:(i + 1) * HIGH]
            turn_real, turn_imaginary = tr_ref[k], ti_ref[k]
            work_ref[k, :HIGH, :] = real * turn_real + imaginary * turn_imaginary
            work_ref[k, HIGH:, :] = imaginary * turn_real - real * turn_imaginary
        return carry

    lax.fori_loop(0, LOW // 2, middle, 0)

    def inverse(step, carry):
        rows = pl.ds(pl.multiple_of(step * 8, 8), 8)
        low_rows = pl.ds(pl.multiple_of(step * 8 + HIGH, 8), 8)
        values = [(work_ref[k, rows, :], work_ref[k, low_rows, :]) for k in range(LOW)]
        for j, (real, imaginary) in enumerate(butterfly(values, 1.0)):
            o_ref[j, 0, rows, :] = real
            o_ref[j, 1, rows, :] = imaginary
        return carry

    lax.fori_loop(0, HIGH // 8, inverse, 0)


def columns_step(received, scalars, tables):
    owners, _, height, _ = received.shape
    received = received.reshape(owners, 2, height // HIGH, HIGH, HIGH)
    vmem = pl.BlockSpec(memory_space=pltpu.VMEM)
    return pl.pallas_call(
        column_kernel,
        in_specs=[pl.BlockSpec(memory_space=pltpu.SMEM)] + [vmem] * (1 + len(tables)),
        out_specs=vmem,
        out_shape=jax.ShapeDtypeStruct((LOW, 2, HIGH, HIGH), jnp.float32),
        scratch_shapes=[pltpu.VMEM((LOW, 2 * HIGH, HIGH), jnp.float32)],
        compiler_params=pltpu.CompilerParams(vmem_limit_bytes=VMEM_LIMIT),
        cost_estimate=pl.CostEstimate(flops=12 * LOW * HIGH * 256 * 256 * 2, bytes_accessed=16 * 1024 * 1024, transcendentals=0),
    )(scalars, received, *tables)


def output_kernel(chunks, *refs):
    inputs = refs[:chunks]
    tr_ref, ti_ref, th_ref, tl_ref, o_ref, work_ref = refs[chunks:]
    owners, _, height, _ = inputs[0].shape
    for owner in range(owners):
        for chunk in range(chunks):
            k = chunks * owner + chunk
            value = jnp.concatenate([inputs[chunk][owner, 0], inputs[chunk][owner, 1]], axis=1)
            high, low = split(value)
            out = dot(high, th_ref[...]) + dot(low, th_ref[...]) + dot(high, tl_ref[...])
            real, imaginary = out[:, :HIGH], out[:, HIGH:]
            turn_real, turn_imaginary = tr_ref[k:k + 1, :], ti_ref[k:k + 1, :]
            work_ref[k, 0] = real * turn_real - imaginary * turn_imaginary
            work_ref[k, 1] = real * turn_imaginary + imaginary * turn_real

    def body(step, carry):
        rows = pl.ds(pl.multiple_of(step * 8, 8), 8)
        values = [(work_ref[k, 0, rows, :], work_ref[k, 1, rows, :]) for k in range(LOW)]
        for j, (real, imaginary) in enumerate(butterfly(values, 1.0)):
            o_ref[0, rows, j * HIGH:(j + 1) * HIGH] = real
            o_ref[1, rows, j * HIGH:(j + 1) * HIGH] = imaginary
        return carry

    lax.fori_loop(0, height // 8, body, 0)


def inverse_width(parts, tables):
    height = parts[0].shape[2]
    vmem = pl.BlockSpec(memory_space=pltpu.VMEM)
    return pl.pallas_call(
        functools.partial(output_kernel, len(parts)),
        in_specs=[vmem] * (len(parts) + len(tables)),
        out_specs=vmem,
        out_shape=jax.ShapeDtypeStruct((2, height, N), jnp.float32),
        scratch_shapes=[pltpu.VMEM((LOW, 2, height, HIGH), jnp.float32)],
        compiler_params=pltpu.CompilerParams(vmem_limit_bytes=VMEM_LIMIT),
        cost_estimate=pl.CostEstimate(flops=6 * LOW * height * 256 * 256, bytes_accessed=8 * height * N * 2, transcendentals=0),
        name="output",
    )(*parts, *tables)


def local(target, depth_index, band_mask):
    owners, depths = lax.axis_size("rows"), lax.axis_size("depth")
    chunks = LOW // owners
    field = target.reshape(target.shape[1:])
    scale = 1.0 / math.sqrt(N)
    forward, backward = dense_table(-1.0), dense_table(1.0)
    left = tuple(jnp.concatenate([h, h, l], axis=1) for h, l in (halves(forward), halves(backward)))
    forward_right, backward_right = halves(forward.T), halves(backward.T)
    turn = twiddles(-1.0, scale)
    turn_back = twiddles(1.0, scale / math.sqrt(depths))
    spread = tuple(jnp.broadcast_to(t[:, :, None], (LOW, HIGH, HIGH)) for t in turn)
    limits = (jnp.sum(band_mask[0], axis=-1) + 1) // 2
    me = lax.axis_index("rows")
    rows = N // (owners * depths)

    pieces = []
    for chunk in range(chunks):
        sent = along_width(field, chunk, chunks, owners, turn + forward_right)
        received = lax.all_to_all(sent, "rows", split_axis=0, concat_axis=0, tiled=True)
        scalars = jnp.stack([depth_index[0], limits[0], limits[1], me * chunks + chunk]).astype(jnp.int32)
        part = columns_step(received, scalars, spread + left)
        pieces.append(lax.psum_scatter(part, "depth", scatter_dimension=0, tiled=True))
    results = []
    for share in pieces:
        share = share.reshape(share.shape[0], 2, HIGH // rows, rows, HIGH)
        share = jnp.transpose(share, (0, 2, 1, 3, 4)).reshape(owners, 2, rows, HIGH)
        results.append(lax.all_to_all(share, "rows", split_axis=0, concat_axis=0, tiled=True))
    return inverse_width(results, turn_back + backward_right)


MESH = pl.DeviceIdType.MESH
PART = 16
PARTS = HIGH // PART
LINE_VMEM = 62 * 1024 * 1024
VARIANTS = ((5, 6), (6, 7), (6, 8), (7, 7), (7, 8), (8, 8))


def slots():
    half = PART // 2
    order = []
    for part in range(PARTS):
        order += list(range(half * part, half * (part + 1)))
        order += list(range(HIGH - half * (part + 1), HIGH - half * part))
    return np.array(order)


def both(index):
    return np.concatenate([index, index + HIGH])


def nt_dot(left, right):
    return lax.dot_general(left, right, (((1,), (1,)), ((), ())), preferred_element_type=jnp.float32)


def width_rows(chunk, chunks, owners, x_at, rows, target, tr_ref, ti_ref, v_ref):
    values = []
    for first in range(owners):
        total = None
        for second in range(chunks):
            at = (first + owners * second) * HIGH
            value = scaled((x_at(0, rows, at), x_at(1, rows, at)), *root(chunk * second, chunks, -1.0))
            total = value if total is None else add(total, value)
        values.append(scaled(total, *root(chunk * first, LOW, -1.0)))
    for owner, (real, imaginary) in enumerate(butterfly(values, -1.0)):
        k = chunks * owner + chunk
        turn_real, turn_imaginary = tr_ref[k:k + 1, :], ti_ref[k:k + 1, :]
        v_ref[owner, target, :HIGH] = real * turn_real - imaginary * turn_imaginary
        v_ref[owner, target, HIGH:] = real * turn_imaginary + imaginary * turn_real


def width_dense(step, th_ref, tl_ref, v_ref, put):
    value = jnp.concatenate([v_ref[2 * step], v_ref[2 * step + 1]], axis=0)
    high, low = split(value)
    out = nt_dot(th_ref[...], high) + nt_dot(th_ref[...], low) + nt_dot(tl_ref[...], high)
    for i in range(2):
        for part in range(PARTS):
            for side in range(2):
                at = side * HIGH + part * PART
                put(part, 2 * step + i, side, out[at:at + PART, i * HIGH:(i + 1) * HIGH])


def spread_kernel(chunks, owners, depths, depth_ref, mask_ref, x_ref, tr_ref, ti_ref, th_ref, tl_ref, o_ref, scalars_ref, choice_ref,
                  v_ref, limit_ref, landing, send, recv):
    here, me = lax.axis_index("depth"), lax.axis_index("rows")
    tile = pl.program_id(0)

    def limit_copy(step):
        return pltpu.make_async_remote_copy(
            src_ref=limit_ref,
            dst_ref=landing.at[here],
            send_sem=send,
            recv_sem=recv,
            device_id=((here + step) % depths, me),
            device_id_type=MESH,
        )

    def sum_of_limits(sem):
        some = landing.at[pl.ds(0, depths - 1)]
        return pltpu.make_async_copy(some, some, sem)

    @pl.when(tile == 0)
    def _():
        barrier = pltpu.get_barrier_semaphore()
        for step in range(1, depths):
            pl.semaphore_signal(barrier, inc=1, device_id=((here + step) % depths, me), device_id_type=MESH)
        ones = mask_ref[0].astype(jnp.float32)
        height, width = [(jnp.sum(ones[side:side + 1, :]) + 1.0) * 0.5 for side in range(2)]
        scalars_ref[0] = depth_ref[0]
        scalars_ref[1] = height.astype(jnp.int32)
        scalars_ref[2] = width.astype(jnp.int32)
        limit_ref[...] = jnp.full(limit_ref.shape, width)
        landing[here] = jnp.full(limit_ref.shape, width)
        pl.semaphore_wait(barrier, depths - 1)
        for step in range(1, depths):
            limit_copy(step).start()

    def body(step, carry):
        rows = pl.ds(pl.multiple_of(step * 8, 8), 8)
        width_rows(0, chunks, owners, lambda side, r, at: x_ref[side, r, at:at + HIGH], rows, rows, tr_ref, ti_ref, v_ref)
        return carry

    lax.fori_loop(0, HIGH // 8, body, 0)

    def put(part, owner, side, value):
        o_ref[part, owner, 0, side] = value

    def dense(step, carry):
        width_dense(step, th_ref, tl_ref, v_ref, put)
        return carry

    lax.fori_loop(0, owners // 2, dense, 0, unroll=True)

    @pl.when(tile == pl.num_programs(0) - 1)
    def _():
        sum_of_limits(recv).wait()
        sum_of_limits(send).wait()
        widths = [jnp.max(landing[q]) for q in range(depths)]
        outer, most = jnp.maximum(widths[0], widths[-1]), functools.reduce(jnp.maximum, widths)
        reach = LOW * PART // 2
        missed, fits = jnp.int32(0), jnp.bool_(False)
        for a, b in VARIANTS[:-1]:
            fits = jnp.logical_or(fits, jnp.logical_and(outer <= a * reach, most <= b * reach))
            missed = missed + jnp.where(fits, 0, 1)
        choice_ref[0] = missed
        choice_ref[1] = sum(jnp.where(most > part * reach, 1, 0) for part in range(PARTS))


def spread_width(field, depth_index, band_mask, chunks, owners, depths, tables):
    _, height, _ = field.shape
    whole = lambda a: pl.BlockSpec(a.shape, lambda i: (0,) * a.ndim)
    smem = pl.BlockSpec(memory_space=pltpu.SMEM)
    shape = (PARTS, owners, height // HIGH, 2, PART, HIGH)
    return pl.pallas_call(
        functools.partial(spread_kernel, chunks, owners, depths),
        grid=(height // HIGH,),
        in_specs=[smem, pl.BlockSpec(memory_space=pltpu.VMEM), pl.BlockSpec((2, HIGH, N), lambda i: (0, i, 0))] + [whole(a) for a in tables],
        out_specs=[
            pl.BlockSpec(shape[:2] + (1,) + shape[3:], lambda i: (0, 0, i, 0, 0, 0)),
            smem,
            smem,
        ],
        out_shape=[jax.ShapeDtypeStruct(shape, jnp.float32), jax.ShapeDtypeStruct((3,), jnp.int32), jax.ShapeDtypeStruct((2,), jnp.int32)],
        scratch_shapes=[
            pltpu.VMEM((owners, HIGH, 2 * HIGH), jnp.float32),
            pltpu.VMEM((8, HIGH), jnp.float32),
            pltpu.VMEM((depths, 8, HIGH), jnp.float32),
            pltpu.SemaphoreType.DMA,
            pltpu.SemaphoreType.DMA,
        ],
        compiler_params=pltpu.CompilerParams(vmem_limit_bytes=VMEM_LIMIT, collective_id=0, has_side_effects=True),
        name="spread",
    )(depth_index, band_mask, field, *tables)


def line_kernel(chunks, owners, depths, outer, levels, scalars_ref, tr_ref, ti_ref, th_ref, tl_ref, fh_ref, fl_ref, ih_ref, il_ref,
                sent_ref, x_ref, back_ref, buf, zbuf, stage, xbuf, v_ref, work_ref,
                self_f, send_f, recv_f, send_r, recv_r, send_l, recv_l, self_b, send_b, recv_b, x_sem):
    total = chunks * levels
    block = LOW // depths
    pieces = LOW // owners
    ahead = max(1, levels - pieces)
    halves_all = (chunks - 1) * pieces * 2
    tall = HIGH // 2
    here, me = lax.axis_index("depth"), lax.axis_index("rows")
    last = depths - 1 - here
    inner = jnp.minimum(here, 1) * jnp.minimum(last, 1)
    mine = outer + (levels - outer) * inner

    def active(t):
        return t % levels < mine

    def filled(t):
        return t % levels < outer

    def when(*conditions):
        return pl.when(functools.reduce(jnp.logical_and, conditions))

    def x_copy(h):
        return pltpu.make_async_copy(x_ref.at[:, pl.ds((h % (2 * pieces)) * tall, tall), :], xbuf.at[h % 2], x_sem.at[h % 2])

    for h in range(min(2, halves_all)):
        x_copy(h).start()

    barrier = pltpu.get_barrier_semaphore()
    for step in range(1, owners):
        pl.semaphore_signal(barrier, inc=1, device_id=(here, (me + step) % owners), device_id_type=MESH)

    @pl.when(here > 0)
    def _():
        pl.semaphore_signal(barrier, inc=1, device_id=(here - 1, me), device_id_type=MESH)

    @pl.when(last > 0)
    def _():
        pl.semaphore_signal(barrier, inc=1, device_id=(here + 1, me), device_id_type=MESH)

    pl.semaphore_wait(barrier, owners - 1 + jnp.minimum(here, 1) + jnp.minimum(last, 1))

    def forward_copies(source, t):
        pltpu.make_async_copy(source.at[me], buf.at[t, pl.ds(me * pieces, pieces)], self_f.at[t]).start()
        for step in range(1, owners):
            peer = (me + step) % owners
            pltpu.make_async_remote_copy(
                src_ref=source.at[peer],
                dst_ref=buf.at[t, pl.ds(me * pieces, pieces)],
                send_sem=send_f.at[t],
                recv_sem=recv_f.at[t],
                device_id=(here, peer),
                device_id_type=MESH,
            ).start()

    def start_forward(t):
        group, part = t // levels, t % levels

        @when(active(t), group == 0)
        def _():
            forward_copies(sent_ref.at[part], t)

        @when(active(t), group > 0)
        def _():
            forward_copies(stage.at[(group + 1) % 2, part], t)

    def arrived(t):
        some = buf.at[t, pl.ds(me * pieces, pieces)]
        return pltpu.make_async_copy(some, some, self_f.at[t])

    def others(t, sem):
        some = buf.at[t, pl.ds(0, pieces * (owners - 1))]
        return pltpu.make_async_copy(some, some, sem.at[t])

    def right_copy(t, q):
        return pltpu.make_async_remote_copy(
            src_ref=buf.at[t, pl.ds(q * block, block)],
            dst_ref=zbuf.at[t, q - here - 1],
            send_sem=send_r.at[t, q - 1],
            recv_sem=recv_r.at[t, q - 1],
            device_id=(here + 1, me),
            device_id_type=MESH,
        )

    def left_copy(t, q):
        return pltpu.make_async_remote_copy(
            src_ref=buf.at[t, pl.ds(q * block, block)],
            dst_ref=zbuf.at[t, depths - here + 1 + q],
            send_sem=send_l.at[t, q],
            recv_sem=recv_l.at[t, q],
            device_id=(here - 1, me),
            device_id_type=MESH,
        )

    def landed(t, at, sem):
        some = zbuf.at[t, at]
        return pltpu.make_async_copy(some, some, sem)

    def final_place(t):
        return back_ref.at[(t // levels) * PARTS + t % levels]

    def final_copy(t, peer):
        return pltpu.make_async_remote_copy(
            src_ref=buf.at[t, here * block + peer],
            dst_ref=final_place(t).at[me],
            send_sem=send_b.at[t],
            recv_sem=recv_b.at[t],
            device_id=(here, peer),
            device_id_type=MESH,
        )

    def final_own(t):
        return pltpu.make_async_copy(buf.at[t, here * block + me], final_place(t).at[me], self_b.at[t])

    def finals(t, sem):
        some = final_place(t).at[pl.ds(0, owners - 1)]
        return pltpu.make_async_copy(some, some, sem.at[t])

    distance = scalars_ref[0].astype(jnp.float32) * 2.0 + 100.0
    limit_height = scalars_ref[1].astype(jnp.float32)
    limit_width = scalars_ref[2].astype(jnp.float32)

    def columns(t):
        def forward(step, carry):
            rows = pl.ds(pl.multiple_of(step * 8, 8), 8)
            values = [(buf[t, p, 0, rows, :], buf[t, p, 1, rows, :]) for p in range(LOW)]
            for k, (real, imaginary) in enumerate(butterfly(values, -1.0)):
                work_ref[k, 0, rows, :] = real
                work_ref[k, 1, rows, :] = imaginary
            return carry

        lax.fori_loop(0, PART // 8, forward, 0)

        column = me * chunks + t // levels
        part = t % levels
        half = PART // 2
        slot = lax.broadcasted_iota(jnp.int32, (PART, HIGH), 0)
        turn = jnp.where(slot < half, half * part + slot, slot - half - half * (part + 1))
        across = (column + LOW * turn).astype(jnp.float32)
        inside_width = jnp.abs(across) < limit_width
        across_square = (across * (1.0 / N)) ** 2
        lanes = lax.broadcasted_iota(jnp.int32, (1, HIGH), 1) * LOW
        group = 16

        def middle(step, carry):
            taken = []
            for i in range(group):
                k = group * step + i
                real, imaginary = work_ref[k, 0], work_ref[k, 1]
                turn_real, turn_imaginary = tr_ref[pl.ds(k, 1), :], ti_ref[pl.ds(k, 1), :]
                taken.append(jnp.concatenate(
                    [real * turn_real - imaginary * turn_imaginary, real * turn_imaginary + imaginary * turn_real], axis=1))
            high, low = split(jnp.concatenate(taken, axis=0))
            spectrum = dot(high, fh_ref[...]) + dot(low, fh_ref[...]) + dot(high, fl_ref[...])
            moved = []
            for i in range(group):
                real, imaginary = spectrum[i * PART:(i + 1) * PART, :HIGH], spectrum[i * PART:(i + 1) * PART, HIGH:]
                down = signed(lanes + (group * step + i))
                square = (down * (1.0 / N)) ** 2 + across_square
                rest_square = 4.0 - square
                drop = 2.0 - rest_square * lax.rsqrt(rest_square)
                turns = -distance * (0.25 * (square + drop * drop))
                rest = turns - jnp.floor(turns + 0.5)
                at = rest * rest
                keep = jnp.logical_and(jnp.abs(down) < limit_height, inside_width)
                cosine = jnp.where(keep, horner(COSINE, at), 0.0)
                sine = jnp.where(keep, horner(SINE, at) * rest, 0.0)
                moved.append(jnp.concatenate([real * cosine - imaginary * sine, real * sine + imaginary * cosine], axis=1))
            high, low = split(jnp.concatenate(moved, axis=0))
            back = dot(high, ih_ref[...]) + dot(low, ih_ref[...]) + dot(high, il_ref[...])
            for i in range(group):
                k = group * step + i
                real, imaginary = back[i * PART:(i + 1) * PART, :HIGH], back[i * PART:(i + 1) * PART, HIGH:]
                turn_real, turn_imaginary = tr_ref[pl.ds(k, 1), :], ti_ref[pl.ds(k, 1), :]
                work_ref[k, 0] = real * turn_real + imaginary * turn_imaginary
                work_ref[k, 1] = imaginary * turn_real - real * turn_imaginary
            return carry

        lax.fori_loop(0, LOW // group, middle, 0)

        def inverse(step, carry):
            rows = pl.ds(pl.multiple_of(step * 8, 8), 8)
            values = [(work_ref[k, 0, rows, :], work_ref[k, 1, rows, :]) for k in range(LOW)]
            for j, (real, imaginary) in enumerate(butterfly(values, 1.0)):
                buf[t, j, 0, rows, :] = real
                buf[t, j, 1, rows, :] = imaginary
            return carry

        lax.fori_loop(0, PART // 8, inverse, 0)

    def merge(t, q, at):
        @pl.when(active(t))
        def _():
            def body(j, carry):
                buf[t, q * block + j] += zbuf[t, at, j]
                return carry

            lax.fori_loop(0, block, body, 0)

        if outer < levels:
            @pl.when(jnp.logical_not(active(t)))
            def _():
                def body(j, carry):
                    buf[t, q * block + j] = zbuf[t, at, j]
                    return carry

                lax.fori_loop(0, block, body, 0)

    def width_tile(chunk, piece):
        for half in range(2):
            h = ((chunk - 1) * pieces + piece) * 2 + half
            x_copy(h).wait()

            def body(step, carry):
                rows = pl.ds(pl.multiple_of(step * 8, 8), 8)
                target = pl.ds(pl.multiple_of(step * 8 + half * tall, 8), 8)
                width_rows(chunk, chunks, owners, lambda side, r, at: xbuf[half, side, r, at:at + HIGH], rows, target, tr_ref, ti_ref, v_ref)
                return carry

            lax.fori_loop(0, tall // 8, body, 0)

            @pl.when(h + 2 < halves_all)
            def _():
                x_copy(h + 2).start()

        def put(part, owner, side, value):
            if isinstance(part, int) and part >= levels:
                return
            stage[(chunk + 1) % 2, part, owner, piece, side] = value

        def dense(step, carry):
            width_dense(step, th_ref, tl_ref, v_ref, put)
            return carry

        lax.fori_loop(0, owners // 2, dense, 0)

    def begin(t, carry):
        start_forward(t)
        return carry

    lax.fori_loop(0, min(ahead, total), begin, 0)

    def step(t, carry):
        @pl.when(t + ahead < total)
        def _():
            start_forward(t + ahead)

        @when(t < total, active(t))
        def _():
            arrived(t).wait()
            others(t, recv_f).wait()
            columns(t)

        right = t - here

        @when(right >= 0, right < total)
        def _():
            for q in range(depths - 1, 0, -1):
                @when(here > 0, q >= here, jnp.logical_or(here > 1, filled(right)))
                def _():
                    landed(right, q - here, recv_r.at[right, q - 1]).wait()
                    merge(right, q, q - here)

                @when(q > here, jnp.logical_or(here > 0, filled(right)))
                def _():
                    right_copy(right, q).start()

        left = t - last

        @when(left >= 0, left < total)
        def _():
            for q in range(depths - 1):
                @when(last > 0, q <= here, jnp.logical_or(last > 1, filled(left)))
                def _():
                    landed(left, depths - here + q, recv_l.at[left, q]).wait()
                    merge(left, q, depths - here + q)

                @when(q < here, jnp.logical_or(last > 0, filled(left)))
                def _():
                    left_copy(left, q).start()

        done = t - jnp.maximum(here, last)

        @when(done >= 0, done < total)
        def _():
            final_own(done).start()
            for step in range(1, owners):
                final_copy(done, (me + step) % owners).start()

        group, piece = t // levels, t % levels
        for chunk in range(1, chunks):
            @when(group == chunk - 1, piece < pieces)
            def _():
                if chunk > 2:
                    @pl.when(piece == 0)
                    def _():
                        def free(part, carry):
                            @pl.when(active(part))
                            def _():
                                others((chunk - 2) * levels + part, send_f).wait()

                            return carry

                        lax.fori_loop(0, levels, free, 0)
                width_tile(chunk, piece)

        return carry

    lax.fori_loop(0, total + depths - 1, step, 0)

    def finish(t, carry):
        group = t // levels

        @when(active(t), jnp.logical_or(group == 0, group + 2 >= chunks))
        def _():
            others(t, send_f).wait()

        for q in range(1, depths):
            @when(q > here, jnp.logical_or(here > 0, filled(t)))
            def _():
                right_copy(t, q).wait_send()
        for q in range(depths - 1):
            @when(q < here, jnp.logical_or(last > 0, filled(t)))
            def _():
                left_copy(t, q).wait_send()
        final_own(t).wait()
        finals(t, send_b).wait()
        finals(t, recv_b).wait()
        return carry

    lax.fori_loop(0, total, finish, 0)


def line(variant, chunks, owners, depths, sent, field, scalars, *tables):
    outer, levels = VARIANTS[variant]
    total = chunks * levels
    block = LOW // depths
    pieces = LOW // owners
    vmem = pl.BlockSpec(memory_space=pltpu.VMEM)
    hbm = pl.BlockSpec(memory_space=pl.ANY)
    dma = pltpu.SemaphoreType.DMA
    tile = (2, PART, HIGH)
    return pl.pallas_call(
        functools.partial(line_kernel, chunks, owners, depths, outer, levels),
        in_specs=[pl.BlockSpec(memory_space=pltpu.SMEM)] + [vmem] * len(tables) + [hbm, hbm],
        out_specs=hbm,
        out_shape=jax.ShapeDtypeStruct((chunks * PARTS, owners) + tile, jnp.float32),
        scratch_shapes=[
            pltpu.VMEM((total, LOW) + tile, jnp.float32),
            pltpu.VMEM((total, depths + 1, block) + tile, jnp.float32),
            pltpu.VMEM((2, levels, owners, pieces) + tile, jnp.float32),
            pltpu.VMEM((2, 2, HIGH // 2, N), jnp.float32),
            pltpu.VMEM((owners, HIGH, 2 * HIGH), jnp.float32),
            pltpu.VMEM((LOW,) + tile, jnp.float32),
            dma((total,)), dma((total,)), dma((total,)),
            dma((total, depths - 1)), dma((total, depths - 1)),
            dma((total, depths - 1)), dma((total, depths - 1)),
            dma((total,)), dma((total,)), dma((total,)),
            dma((2,)),
        ],
        compiler_params=pltpu.CompilerParams(vmem_limit_bytes=LINE_VMEM, collective_id=1 + variant, has_side_effects=True),
    )(scalars, *tables, sent, field)


def gather_kernel(chunks, levels_ref, in_ref, tr_ref, ti_ref, th_ref, tl_ref, o_ref, work_ref):
    levels = levels_ref[1]

    def dense(k, carry):
        owner, chunk = k // chunks, k % chunks
        sides = [
            jnp.concatenate([
                jnp.where(part < levels, in_ref[chunk * PARTS + part, owner, side], 0.0) for part in range(PARTS)
            ], axis=0).T
            for side in range(2)
        ]
        high, low = split(jnp.concatenate(sides, axis=1))
        out = dot(high, th_ref[...]) + dot(low, th_ref[...]) + dot(high, tl_ref[...])
        real, imaginary = out[:, :HIGH], out[:, HIGH:]
        turn_real, turn_imaginary = tr_ref[pl.ds(k, 1), :], ti_ref[pl.ds(k, 1), :]
        work_ref[k, 0] = real * turn_real - imaginary * turn_imaginary
        work_ref[k, 1] = real * turn_imaginary + imaginary * turn_real
        return carry

    lax.fori_loop(0, LOW, dense, 0, unroll=4)

    def body(step, carry):
        rows = pl.ds(pl.multiple_of(step * 8, 8), 8)
        values = [(work_ref[k, 0, rows, :], work_ref[k, 1, rows, :]) for k in range(LOW)]
        for j, (real, imaginary) in enumerate(butterfly(values, 1.0)):
            o_ref[0, rows, j * HIGH:(j + 1) * HIGH] = real
            o_ref[1, rows, j * HIGH:(j + 1) * HIGH] = imaginary
        return carry

    lax.fori_loop(0, HIGH // 8, body, 0)


def gather_width(parts, levels, chunks, tables):
    vmem = pl.BlockSpec(memory_space=pltpu.VMEM)
    return pl.pallas_call(
        functools.partial(gather_kernel, chunks),
        in_specs=[pl.BlockSpec(memory_space=pltpu.SMEM)] + [vmem] * (1 + len(tables)),
        out_specs=vmem,
        out_shape=jax.ShapeDtypeStruct((2, HIGH, N), jnp.float32),
        scratch_shapes=[pltpu.VMEM((LOW, 2, HIGH, HIGH), jnp.float32)],
        compiler_params=pltpu.CompilerParams(vmem_limit_bytes=VMEM_LIMIT),
        name="gather",
    )(levels, parts, *tables)


def fused(target, depth_index, band_mask):
    owners, depths = lax.axis_size("rows"), lax.axis_size("depth")
    chunks = LOW // owners
    field = target.reshape(target.shape[1:])
    scale = 1.0 / math.sqrt(N)
    forward, backward = dense_table(-1.0), dense_table(1.0)
    order = both(slots())
    turn = twiddles(-1.0, scale)
    turn_back = twiddles(1.0, scale / math.sqrt(depths))
    wide = halves(forward[order])
    sent, scalars, choice = spread_width(field, depth_index, band_mask, chunks, owners, depths, turn + wide)
    choices = [functools.partial(line, i, chunks, owners, depths) for i in range(len(VARIANTS))]
    tables = turn + wide + halves(forward.T) + halves(backward.T)
    parts = lax.switch(choice[0], choices, sent, field, scalars, *tables)
    return gather_width(parts, choice, chunks, turn_back + halves(backward.T[order]))


def solution(mesh):
    in_specs = (P("depth", None, "rows", None), P("depth"), P("depth", None, None))
    out_specs = P(None, ("depth", "rows"), None)
    step = jax.shard_map(local, mesh=mesh, in_specs=in_specs, out_specs=out_specs, check_vma=False)
    if mesh.shape["rows"] * mesh.shape["depth"] == LOW and mesh.shape["depth"] > 1:
        return jax.shard_map(fused, mesh=mesh, in_specs=in_specs, out_specs=out_specs, check_vma=False)
    return step
```

```python
import functools
import math

import jax
import jax.numpy as jnp
import numpy as np
from jax import lax
from jax.experimental import pallas as pl
from jax.experimental.pallas import tpu as pltpu
from jax.sharding import PartitionSpec as P


LOW = 32
HIGH = 128
N = LOW * HIGH
VMEM_LIMIT = 56 * 1024 * 1024


def scaled(value, factor_real, factor_imaginary):
    real, imaginary = value
    if abs(factor_imaginary) < 1e-12:
        if factor_real > 0:
            return (real, imaginary)
        return (-real, -imaginary)
    if abs(factor_real) < 1e-12:
        if factor_imaginary > 0:
            return (-imaginary, real)
        return (imaginary, -real)
    a, b = np.float32(factor_real), np.float32(factor_imaginary)
    return (real * a - imaginary * b, real * b + imaginary * a)


def root(numerator, length, direction):
    angle = direction * 2.0 * math.pi * (numerator % length) / length
    return math.cos(angle), math.sin(angle)


def add(left, right):
    return (left[0] + right[0], left[1] + right[1])


def subtract(left, right):
    return (left[0] - right[0], left[1] - right[1])


def butterfly(values, direction):
    count = len(values)
    if count == 1:
        return values
    even = butterfly(values[0::2], direction)
    odd = butterfly(values[1::2], direction)
    odd = [scaled(v, *root(k, count, direction)) for k, v in enumerate(odd)]
    return [add(e, o) for e, o in zip(even, odd)] + [subtract(e, o) for e, o in zip(even, odd)]


def dense_table(direction):
    index = np.arange(HIGH)
    angles = direction * 2.0 * np.pi / HIGH * (index[:, None] * index[None, :] % HIGH)
    cosine, sine = np.cos(angles), np.sin(angles)
    return np.block([[cosine, -sine], [sine, cosine]])


def halves(table):
    high = table.astype(np.float32).astype(jnp.bfloat16)
    low = (table - high.astype(np.float64)).astype(np.float32).astype(jnp.bfloat16)
    return jnp.asarray(high), jnp.asarray(low)


def twiddles(direction, scaling):
    product = np.arange(LOW)[:, None] * np.arange(HIGH)[None, :] % N
    angles = direction * 2.0 * np.pi / N * product
    return (
        jnp.asarray((np.cos(angles) * scaling).astype(np.float32)),
        jnp.asarray((np.sin(angles) * scaling).astype(np.float32)),
    )


def split(value):
    high = value.astype(jnp.bfloat16)
    return high, (value - high.astype(jnp.float32)).astype(jnp.bfloat16)


def tripled(value):
    high, low = split(value)
    return jnp.concatenate([high, low, high], axis=0)


def dot(left, right):
    return jnp.dot(left, right, preferred_element_type=jnp.float32)


def width_kernel(chunk, chunks, owners, x_ref, tr_ref, ti_ref, th_ref, tl_ref, o_ref, hi_ref, lo_ref):
    tile = x_ref.shape[1]

    def body(step, carry):
        rows = pl.ds(pl.multiple_of(step * 16, 16), 16)
        values = []
        for first in range(owners):
            total = None
            for second in range(chunks):
                at = (first + owners * second) * HIGH
                value = (x_ref[0, rows, at:at + HIGH], x_ref[1, rows, at:at + HIGH])
                value = scaled(value, *root(chunk * second, chunks, -1.0))
                total = value if total is None else add(total, value)
            values.append(scaled(total, *root(chunk * first, LOW, -1.0)))
        for owner, (real, imaginary) in enumerate(butterfly(values, -1.0)):
            k = chunks * owner + chunk
            turn_real, turn_imaginary = tr_ref[k:k + 1, :], ti_ref[k:k + 1, :]
            high, low = split(real * turn_real - imaginary * turn_imaginary)
            hi_ref[owner, rows, :HIGH] = high
            lo_ref[owner, rows, :HIGH] = low
            high, low = split(real * turn_imaginary + imaginary * turn_real)
            hi_ref[owner, rows, HIGH:] = high
            lo_ref[owner, rows, HIGH:] = low
        return carry

    lax.fori_loop(0, tile // 16, body, 0)
    for owner in range(owners):
        high = hi_ref[owner]
        out = dot(high, th_ref[...]) + dot(lo_ref[owner], th_ref[...]) + dot(high, tl_ref[...])
        o_ref[owner, 0] = out[:, :HIGH]
        o_ref[owner, 1] = out[:, HIGH:]


def along_width(field, chunk, chunks, owners, tables):
    _, height, _ = field.shape
    tile = min(128, height)
    whole = lambda a: pl.BlockSpec(a.shape, lambda i: (0,) * a.ndim)
    return pl.pallas_call(
        functools.partial(width_kernel, chunk, chunks, owners),
        grid=(height // tile,),
        in_specs=[pl.BlockSpec((2, tile, N), lambda i: (0, i, 0))] + [whole(a) for a in tables],
        out_specs=pl.BlockSpec((owners, 2, tile, HIGH), lambda i: (0, 0, i, 0)),
        out_shape=jax.ShapeDtypeStruct((owners, 2, height, HIGH), jnp.float32),
        scratch_shapes=[pltpu.VMEM((owners, tile, 2 * HIGH), jnp.bfloat16)] * 2,
        compiler_params=pltpu.CompilerParams(vmem_limit_bytes=VMEM_LIMIT),
        cost_estimate=pl.CostEstimate(flops=6 * height * HIGH * HIGH * 4 * owners * 2, bytes_accessed=field.size * 4 + field.size * 4 // chunks, transcendentals=0),
    )(field, *tables)


def series(values, points):
    nodes = np.cos(np.pi * (np.arange(400) + 0.5) / 400) * 0.125 + 0.125
    basis = np.polynomial.chebyshev.Chebyshev.fit(nodes, values(np.sqrt(nodes)), points, domain=[0.0, 0.25])
    return [np.float32(c) for c in basis.convert(kind=np.polynomial.Polynomial).coef]


COSINE = series(lambda r: np.cos(2.0 * np.pi * r), 6)
SINE = series(lambda r: np.sin(2.0 * np.pi * r) / r, 6)


def horner(coefficients, at):
    total = coefficients[-1]
    for c in coefficients[-2::-1]:
        total = total * at + c
    return total


def signed(natural):
    return jnp.where(natural < N // 2, natural, natural - N).astype(jnp.float32)


def column_kernel(scalars_ref, x_ref, tr_ref, ti_ref, f_ref, i_ref, o_ref, work_ref):
    owners, _, pieces, _, _ = x_ref.shape
    distance = scalars_ref[0].astype(jnp.float32) * 2.0 + 100.0
    limit_height = scalars_ref[1].astype(jnp.float32)
    limit_width = scalars_ref[2].astype(jnp.float32)
    column = scalars_ref[3]

    def forward(step, carry):
        rows = pl.ds(pl.multiple_of(step * 8, 8), 8)
        low_rows = pl.ds(pl.multiple_of(step * 8 + HIGH, 8), 8)
        values = [(x_ref[s, 0, p, rows, :], x_ref[s, 1, p, rows, :]) for s in range(owners) for p in range(pieces)]
        for k, (real, imaginary) in enumerate(butterfly(values, -1.0)):
            work_ref[k, rows, :] = real
            work_ref[k, low_rows, :] = imaginary
        return carry

    lax.fori_loop(0, HIGH // 8, forward, 0)

    across = signed(lax.broadcasted_iota(jnp.int32, (1, HIGH), 1) * LOW + column)
    inside_width = jnp.abs(across) < limit_width
    across_square = (across * (1.0 / N)) ** 2

    def turned(k):
        real, imaginary = work_ref[k, :HIGH, :], work_ref[k, HIGH:, :]
        turn_real, turn_imaginary = tr_ref[k], ti_ref[k]
        return jnp.concatenate(
            [real * turn_real - imaginary * turn_imaginary, real * turn_imaginary + imaginary * turn_real], axis=0
        )

    def propagate(k, real, imaginary):
        down = signed(lax.broadcasted_iota(jnp.int32, (HIGH, HIGH), 0) * LOW + k)
        square = (down * (1.0 / N)) ** 2 + across_square
        rest_square = 4.0 - square
        drop = 2.0 - rest_square * lax.rsqrt(rest_square)
        turns = -distance * (0.25 * (square + drop * drop))
        rest = turns - jnp.floor(turns + 0.5)
        at = rest * rest
        keep = jnp.logical_and(jnp.abs(down) < limit_height, inside_width)
        cosine = jnp.where(keep, horner(COSINE, at), 0.0)
        sine = jnp.where(keep, horner(SINE, at) * rest, 0.0)
        return jnp.concatenate([real * cosine - imaginary * sine, real * sine + imaginary * cosine], axis=0)

    def middle(step, carry):
        pair = [2 * step, 2 * step + 1]
        spectrum = dot(f_ref[...], tripled(jnp.concatenate([turned(k) for k in pair], axis=1)))
        moved = [
            propagate(k, spectrum[:HIGH, i * HIGH:(i + 1) * HIGH], spectrum[HIGH:, i * HIGH:(i + 1) * HIGH])
            for i, k in enumerate(pair)
        ]
        back = dot(i_ref[...], tripled(jnp.concatenate(moved, axis=1)))
        for i, k in enumerate(pair):
            real, imaginary = back[:HIGH, i * HIGH:(i + 1) * HIGH], back[HIGH:, i * HIGH:(i + 1) * HIGH]
            turn_real, turn_imaginary = tr_ref[k], ti_ref[k]
            work_ref[k, :HIGH, :] = real * turn_real + imaginary * turn_imaginary
            work_ref[k, HIGH:, :] = imaginary * turn_real - real * turn_imaginary
        return carry

    lax.fori_loop(0, LOW // 2, middle, 0)

    def inverse(step, carry):
        rows = pl.ds(pl.multiple_of(step * 8, 8), 8)
        low_rows = pl.ds(pl.multiple_of(step * 8 + HIGH, 8), 8)
        values = [(work_ref[k, rows, :], work_ref[k, low_rows, :]) for k in range(LOW)]
        for j, (real, imaginary) in enumerate(butterfly(values, 1.0)):
            o_ref[j, 0, rows, :] = real
            o_ref[j, 1, rows, :] = imaginary
        return carry

    lax.fori_loop(0, HIGH // 8, inverse, 0)


def columns_step(received, scalars, tables):
    owners, _, height, _ = received.shape
    received = received.reshape(owners, 2, height // HIGH, HIGH, HIGH)
    vmem = pl.BlockSpec(memory_space=pltpu.VMEM)
    return pl.pallas_call(
        column_kernel,
        in_specs=[pl.BlockSpec(memory_space=pltpu.SMEM)] + [vmem] * (1 + len(tables)),
        out_specs=vmem,
        out_shape=jax.ShapeDtypeStruct((LOW, 2, HIGH, HIGH), jnp.float32),
        scratch_shapes=[pltpu.VMEM((LOW, 2 * HIGH, HIGH), jnp.float32)],
        compiler_params=pltpu.CompilerParams(vmem_limit_bytes=VMEM_LIMIT),
        cost_estimate=pl.CostEstimate(flops=12 * LOW * HIGH * 256 * 256 * 2, bytes_accessed=16 * 1024 * 1024, transcendentals=0),
    )(scalars, received, *tables)


def output_kernel(chunks, *refs):
    inputs = refs[:chunks]
    tr_ref, ti_ref, th_ref, tl_ref, o_ref, work_ref = refs[chunks:]
    owners, _, height, _ = inputs[0].shape
    for owner in range(owners):
        for chunk in range(chunks):
            k = chunks * owner + chunk
            value = jnp.concatenate([inputs[chunk][owner, 0], inputs[chunk][owner, 1]], axis=1)
            high, low = split(value)
            out = dot(high, th_ref[...]) + dot(low, th_ref[...]) + dot(high, tl_ref[...])
            real, imaginary = out[:, :HIGH], out[:, HIGH:]
            turn_real, turn_imaginary = tr_ref[k:k + 1, :], ti_ref[k:k + 1, :]
            work_ref[k, 0] = real * turn_real - imaginary * turn_imaginary
            work_ref[k, 1] = real * turn_imaginary + imaginary * turn_real

    def body(step, carry):
        rows = pl.ds(pl.multiple_of(step * 8, 8), 8)
        values = [(work_ref[k, 0, rows, :], work_ref[k, 1, rows, :]) for k in range(LOW)]
        for j, (real, imaginary) in enumerate(butterfly(values, 1.0)):
            o_ref[0, rows, j * HIGH:(j + 1) * HIGH] = real
            o_ref[1, rows, j * HIGH:(j + 1) * HIGH] = imaginary
        return carry

    lax.fori_loop(0, height // 8, body, 0)


def inverse_width(parts, tables):
    height = parts[0].shape[2]
    vmem = pl.BlockSpec(memory_space=pltpu.VMEM)
    return pl.pallas_call(
        functools.partial(output_kernel, len(parts)),
        in_specs=[vmem] * (len(parts) + len(tables)),
        out_specs=vmem,
        out_shape=jax.ShapeDtypeStruct((2, height, N), jnp.float32),
        scratch_shapes=[pltpu.VMEM((LOW, 2, height, HIGH), jnp.float32)],
        compiler_params=pltpu.CompilerParams(vmem_limit_bytes=VMEM_LIMIT),
        cost_estimate=pl.CostEstimate(flops=6 * LOW * height * 256 * 256, bytes_accessed=8 * height * N * 2, transcendentals=0),
        name="output",
    )(*parts, *tables)


def local(target, depth_index, band_mask):
    owners, depths = lax.axis_size("rows"), lax.axis_size("depth")
    chunks = LOW // owners
    field = target.reshape(target.shape[1:])
    scale = 1.0 / math.sqrt(N)
    forward, backward = dense_table(-1.0), dense_table(1.0)
    left = tuple(jnp.concatenate([h, h, l], axis=1) for h, l in (halves(forward), halves(backward)))
    forward_right, backward_right = halves(forward.T), halves(backward.T)
    turn = twiddles(-1.0, scale)
    turn_back = twiddles(1.0, scale / math.sqrt(depths))
    spread = tuple(jnp.broadcast_to(t[:, :, None], (LOW, HIGH, HIGH)) for t in turn)
    limits = (jnp.sum(band_mask[0], axis=-1) + 1) // 2
    me = lax.axis_index("rows")
    rows = N // (owners * depths)

    pieces = []
    for chunk in range(chunks):
        sent = along_width(field, chunk, chunks, owners, turn + forward_right)
        received = lax.all_to_all(sent, "rows", split_axis=0, concat_axis=0, tiled=True)
        scalars = jnp.stack([depth_index[0], limits[0], limits[1], me * chunks + chunk]).astype(jnp.int32)
        part = columns_step(received, scalars, spread + left)
        pieces.append(lax.psum_scatter(part, "depth", scatter_dimension=0, tiled=True))
    results = []
    for share in pieces:
        share = share.reshape(share.shape[0], 2, HIGH // rows, rows, HIGH)
        share = jnp.transpose(share, (0, 2, 1, 3, 4)).reshape(owners, 2, rows, HIGH)
        results.append(lax.all_to_all(share, "rows", split_axis=0, concat_axis=0, tiled=True))
    return inverse_width(results, turn_back + backward_right)


MESH = pl.DeviceIdType.MESH
PART = 16
PARTS = HIGH // PART
LINE_VMEM = 62 * 1024 * 1024
HOLD = 8
SLACK = 4
VARIANTS = ((5, 6), (5, 7), (6, 7), (6, 8), (7, 8), (8, 8))


def slots():
    half = PART // 2
    order = []
    for part in range(PARTS):
        order += list(range(half * part, half * (part + 1)))
        order += list(range(HIGH - half * (part + 1), HIGH - half * part))
    return np.array(order)


def both(index):
    return np.concatenate([index, index + HIGH])


def nt_dot(left, right):
    return lax.dot_general(left, right, (((1,), (1,)), ((), ())), preferred_element_type=jnp.float32)


def width_rows(chunk, chunks, owners, x_at, rows, target, tr_ref, ti_ref, v_ref):
    values = []
    for first in range(owners):
        total = None
        for second in range(chunks):
            at = (first + owners * second) * HIGH
            value = scaled((x_at(0, rows, at), x_at(1, rows, at)), *root(chunk * second, chunks, -1.0))
            total = value if total is None else add(total, value)
        values.append(scaled(total, *root(chunk * first, LOW, -1.0)))
    for owner, (real, imaginary) in enumerate(butterfly(values, -1.0)):
        k = chunks * owner + chunk
        turn_real, turn_imaginary = tr_ref[k:k + 1, :], ti_ref[k:k + 1, :]
        v_ref[owner, target, :HIGH] = real * turn_real - imaginary * turn_imaginary
        v_ref[owner, target, HIGH:] = real * turn_imaginary + imaginary * turn_real


def width_dense(step, th_ref, tl_ref, v_ref, put):
    value = jnp.concatenate([v_ref[2 * step], v_ref[2 * step + 1]], axis=0)
    high, low = split(value)
    out = nt_dot(th_ref[...], high) + nt_dot(th_ref[...], low) + nt_dot(tl_ref[...], high)
    for i in range(2):
        for part in range(PARTS):
            for side in range(2):
                at = side * HIGH + part * PART
                put(part, 2 * step + i, side, out[at:at + PART, i * HIGH:(i + 1) * HIGH])


def spread_kernel(chunks, owners, depths, depth_ref, mask_ref, x_ref, tr_ref, ti_ref, th_ref, tl_ref, o_ref, scalars_ref, choice_ref,
                  v_ref, limit_ref, landing, send, recv):
    here, me = lax.axis_index("depth"), lax.axis_index("rows")
    tile = pl.program_id(0)

    def limit_copy(step):
        return pltpu.make_async_remote_copy(
            src_ref=limit_ref,
            dst_ref=landing.at[here],
            send_sem=send,
            recv_sem=recv,
            device_id=((here + step) % depths, me),
            device_id_type=MESH,
        )

    def sum_of_limits(sem):
        some = landing.at[pl.ds(0, depths - 1)]
        return pltpu.make_async_copy(some, some, sem)

    @pl.when(tile == 0)
    def _():
        barrier = pltpu.get_barrier_semaphore()
        for step in range(1, depths):
            pl.semaphore_signal(barrier, inc=1, device_id=((here + step) % depths, me), device_id_type=MESH)
        ones = mask_ref[0].astype(jnp.float32)
        height, width = [(jnp.sum(ones[side:side + 1, :]) + 1.0) * 0.5 for side in range(2)]
        scalars_ref[0] = depth_ref[0]
        scalars_ref[1] = height.astype(jnp.int32)
        scalars_ref[2] = width.astype(jnp.int32)
        limit_ref[...] = jnp.full(limit_ref.shape, width)
        landing[here] = jnp.full(limit_ref.shape, width)
        pl.semaphore_wait(barrier, depths - 1)
        for step in range(1, depths):
            limit_copy(step).start()

    def body(step, carry):
        rows = pl.ds(pl.multiple_of(step * 8, 8), 8)
        width_rows(0, chunks, owners, lambda side, r, at: x_ref[side, r, at:at + HIGH], rows, rows, tr_ref, ti_ref, v_ref)
        return carry

    lax.fori_loop(0, HIGH // 8, body, 0)

    def put(part, owner, side, value):
        o_ref[part, owner, 0, side] = value

    def dense(step, carry):
        width_dense(step, th_ref, tl_ref, v_ref, put)
        return carry

    lax.fori_loop(0, owners // 2, dense, 0, unroll=True)

    @pl.when(tile == pl.num_programs(0) - 1)
    def _():
        sum_of_limits(recv).wait()
        sum_of_limits(send).wait()
        widths = [jnp.max(landing[q]) for q in range(depths)]
        outer, most = jnp.maximum(widths[0], widths[-1]), functools.reduce(jnp.maximum, widths)
        reach = LOW * PART // 2
        missed, fits = jnp.int32(0), jnp.bool_(False)
        for a, b in VARIANTS[:-1]:
            fits = jnp.logical_or(fits, jnp.logical_and(outer <= a * reach, most <= b * reach))
            missed = missed + jnp.where(fits, 0, 1)
        choice_ref[0] = missed
        choice_ref[1] = sum(jnp.where(most > part * reach, 1, 0) for part in range(PARTS))


def spread_width(field, depth_index, band_mask, chunks, owners, depths, tables):
    _, height, _ = field.shape
    whole = lambda a: pl.BlockSpec(a.shape, lambda i: (0,) * a.ndim)
    smem = pl.BlockSpec(memory_space=pltpu.SMEM)
    shape = (PARTS, owners, height // HIGH, 2, PART, HIGH)
    return pl.pallas_call(
        functools.partial(spread_kernel, chunks, owners, depths),
        grid=(height // HIGH,),
        in_specs=[smem, pl.BlockSpec(memory_space=pltpu.VMEM), pl.BlockSpec((2, HIGH, N), lambda i: (0, i, 0))] + [whole(a) for a in tables],
        out_specs=[
            pl.BlockSpec(shape[:2] + (1,) + shape[3:], lambda i: (0, 0, i, 0, 0, 0)),
            smem,
            smem,
        ],
        out_shape=[jax.ShapeDtypeStruct(shape, jnp.float32), jax.ShapeDtypeStruct((3,), jnp.int32), jax.ShapeDtypeStruct((2,), jnp.int32)],
        scratch_shapes=[
            pltpu.VMEM((owners, HIGH, 2 * HIGH), jnp.float32),
            pltpu.VMEM((8, HIGH), jnp.float32),
            pltpu.VMEM((depths, 8, HIGH), jnp.float32),
            pltpu.SemaphoreType.DMA,
            pltpu.SemaphoreType.DMA,
        ],
        compiler_params=pltpu.CompilerParams(vmem_limit_bytes=VMEM_LIMIT, collective_id=0, has_side_effects=True),
        name="spread",
    )(depth_index, band_mask, field, *tables)


def line_kernel(chunks, owners, depths, outer, levels, scalars_ref, tr_ref, ti_ref, th_ref, tl_ref, fh_ref, fl_ref, ih_ref, il_ref,
                sent_ref, x_ref, back_ref, buf, zbuf, stage, xbuf, v_ref, work_ref,
                self_f, send_f, recv_f, send_r, recv_r, send_l, recv_l, self_b, send_b, recv_b, x_sem):
    total = chunks * levels
    block = LOW // depths
    pieces = LOW // owners
    ahead = max(1, levels - pieces)
    halves_all = (chunks - 1) * pieces * 2
    tall = HIGH // 2
    here, me = lax.axis_index("depth"), lax.axis_index("rows")
    last = depths - 1 - here
    inner = jnp.minimum(here, 1) * jnp.minimum(last, 1)
    mine = outer + (levels - outer) * inner

    def active(t):
        return t % levels < mine

    def filled(t):
        return t % levels < outer

    def when(*conditions):
        return pl.when(functools.reduce(jnp.logical_and, conditions))

    def x_copy(h):
        return pltpu.make_async_copy(x_ref.at[:, pl.ds((h % (2 * pieces)) * tall, tall), :], xbuf.at[h % 2], x_sem.at[h % 2])

    for h in range(min(2, halves_all)):
        x_copy(h).start()

    barrier = pltpu.get_barrier_semaphore()
    for step in range(1, owners):
        pl.semaphore_signal(barrier, inc=1, device_id=(here, (me + step) % owners), device_id_type=MESH)

    @pl.when(here > 0)
    def _():
        pl.semaphore_signal(barrier, inc=1, device_id=(here - 1, me), device_id_type=MESH)

    @pl.when(last > 0)
    def _():
        pl.semaphore_signal(barrier, inc=1, device_id=(here + 1, me), device_id_type=MESH)

    pl.semaphore_wait(barrier, owners - 1 + jnp.minimum(here, 1) + jnp.minimum(last, 1))

    def forward_copies(source, t):
        pltpu.make_async_copy(source.at[me], buf.at[t, pl.ds(me * pieces, pieces)], self_f.at[t]).start()
        for step in range(1, owners):
            peer = (me + step) % owners
            pltpu.make_async_remote_copy(
                src_ref=source.at[peer],
                dst_ref=buf.at[t, pl.ds(me * pieces, pieces)],
                send_sem=send_f.at[t],
                recv_sem=recv_f.at[t],
                device_id=(here, peer),
                device_id_type=MESH,
            ).start()

    def start_forward(t):
        group, part = t // levels, t % levels

        @when(active(t), group == 0)
        def _():
            forward_copies(sent_ref.at[part], t)

        @when(active(t), group > 0)
        def _():
            forward_copies(stage.at[(group + 1) % 2, part], t)

    def arrived(t):
        some = buf.at[t, pl.ds(me * pieces, pieces)]
        return pltpu.make_async_copy(some, some, self_f.at[t])

    def others(t, sem):
        some = buf.at[t, pl.ds(0, pieces * (owners - 1))]
        return pltpu.make_async_copy(some, some, sem.at[t])

    def right_copy(t, q):
        return pltpu.make_async_remote_copy(
            src_ref=buf.at[t, pl.ds(q * block, block)],
            dst_ref=zbuf.at[t, q - here - 1],
            send_sem=send_r.at[t, q - 1],
            recv_sem=recv_r.at[t, q - 1],
            device_id=(here + 1, me),
            device_id_type=MESH,
        )

    def left_copy(t, q):
        return pltpu.make_async_remote_copy(
            src_ref=buf.at[t, pl.ds(q * block, block)],
            dst_ref=zbuf.at[t, depths - here + 1 + q],
            send_sem=send_l.at[t, q],
            recv_sem=recv_l.at[t, q],
            device_id=(here - 1, me),
            device_id_type=MESH,
        )

    def landed(t, at, sem):
        some = zbuf.at[t, at]
        return pltpu.make_async_copy(some, some, sem)

    def final_place(t):
        return back_ref.at[(t // levels) * PARTS + t % levels]

    def final_copy(t, peer):
        return pltpu.make_async_remote_copy(
            src_ref=buf.at[t, here * block + peer],
            dst_ref=final_place(t).at[me],
            send_sem=send_b.at[t],
            recv_sem=recv_b.at[t],
            device_id=(here, peer),
            device_id_type=MESH,
        )

    def final_own(t):
        return pltpu.make_async_copy(buf.at[t, here * block + me], final_place(t).at[me], self_b.at[t])

    def finals(t, sem):
        some = final_place(t).at[pl.ds(0, owners - 1)]
        return pltpu.make_async_copy(some, some, sem.at[t])

    distance = scalars_ref[0].astype(jnp.float32) * 2.0 + 100.0
    limit_height = scalars_ref[1].astype(jnp.float32)
    limit_width = scalars_ref[2].astype(jnp.float32)

    def columns(t):
        def forward(step, carry):
            rows = pl.ds(pl.multiple_of(step * 8, 8), 8)
            values = [(buf[t, p, 0, rows, :], buf[t, p, 1, rows, :]) for p in range(LOW)]
            for k, (real, imaginary) in enumerate(butterfly(values, -1.0)):
                work_ref[k, 0, rows, :] = real
                work_ref[k, 1, rows, :] = imaginary
            return carry

        lax.fori_loop(0, PART // 8, forward, 0)

        column = me * chunks + t // levels
        part = t % levels
        half = PART // 2
        slot = lax.broadcasted_iota(jnp.int32, (PART, HIGH), 0)
        turn = jnp.where(slot < half, half * part + slot, slot - half - half * (part + 1))
        across = (column + LOW * turn).astype(jnp.float32)
        inside_width = jnp.abs(across) < limit_width
        across_square = (across * (1.0 / N)) ** 2
        lanes = lax.broadcasted_iota(jnp.int32, (1, HIGH), 1) * LOW
        group = 16

        def middle(step, carry):
            taken = []
            for i in range(group):
                k = group * step + i
                real, imaginary = work_ref[k, 0], work_ref[k, 1]
                turn_real, turn_imaginary = tr_ref[pl.ds(k, 1), :], ti_ref[pl.ds(k, 1), :]
                taken.append(jnp.concatenate(
                    [real * turn_real - imaginary * turn_imaginary, real * turn_imaginary + imaginary * turn_real], axis=1))
            high, low = split(jnp.concatenate(taken, axis=0))
            spectrum = dot(high, fh_ref[...]) + dot(low, fh_ref[...]) + dot(high, fl_ref[...])
            moved = []
            for i in range(group):
                real, imaginary = spectrum[i * PART:(i + 1) * PART, :HIGH], spectrum[i * PART:(i + 1) * PART, HIGH:]
                down = signed(lanes + (group * step + i))
                square = (down * (1.0 / N)) ** 2 + across_square
                rest_square = 4.0 - square
                drop = 2.0 - rest_square * lax.rsqrt(rest_square)
                turns = -distance * (0.25 * (square + drop * drop))
                rest = turns - jnp.floor(turns + 0.5)
                at = rest * rest
                keep = jnp.logical_and(jnp.abs(down) < limit_height, inside_width)
                cosine = jnp.where(keep, horner(COSINE, at), 0.0)
                sine = jnp.where(keep, horner(SINE, at) * rest, 0.0)
                moved.append(jnp.concatenate([real * cosine - imaginary * sine, real * sine + imaginary * cosine], axis=1))
            high, low = split(jnp.concatenate(moved, axis=0))
            back = dot(high, ih_ref[...]) + dot(low, ih_ref[...]) + dot(high, il_ref[...])
            for i in range(group):
                k = group * step + i
                real, imaginary = back[i * PART:(i + 1) * PART, :HIGH], back[i * PART:(i + 1) * PART, HIGH:]
                turn_real, turn_imaginary = tr_ref[pl.ds(k, 1), :], ti_ref[pl.ds(k, 1), :]
                work_ref[k, 0] = real * turn_real + imaginary * turn_imaginary
                work_ref[k, 1] = imaginary * turn_real - real * turn_imaginary
            return carry

        lax.fori_loop(0, LOW // group, middle, 0)

        def inverse(step, carry):
            rows = pl.ds(pl.multiple_of(step * 8, 8), 8)
            values = [(work_ref[k, 0, rows, :], work_ref[k, 1, rows, :]) for k in range(LOW)]
            for j, (real, imaginary) in enumerate(butterfly(values, 1.0)):
                buf[t, j, 0, rows, :] = real
                buf[t, j, 1, rows, :] = imaginary
            return carry

        lax.fori_loop(0, PART // 8, inverse, 0)

    def merge(t, q, at):
        @pl.when(active(t))
        def _():
            def body(j, carry):
                buf[t, q * block + j] += zbuf[t, at, j]
                return carry

            lax.fori_loop(0, block, body, 0)

        if outer < levels:
            @pl.when(jnp.logical_not(active(t)))
            def _():
                def body(j, carry):
                    buf[t, q * block + j] = zbuf[t, at, j]
                    return carry

                lax.fori_loop(0, block, body, 0)

    def width_tile(chunk, piece):
        for half in range(2):
            h = ((chunk - 1) * pieces + piece) * 2 + half
            x_copy(h).wait()

            def body(step, carry):
                rows = pl.ds(pl.multiple_of(step * 8, 8), 8)
                target = pl.ds(pl.multiple_of(step * 8 + half * tall, 8), 8)
                width_rows(chunk, chunks, owners, lambda side, r, at: xbuf[half, side, r, at:at + HIGH], rows, target, tr_ref, ti_ref, v_ref)
                return carry

            lax.fori_loop(0, tall // 8, body, 0)

            @pl.when(h + 2 < halves_all)
            def _():
                x_copy(h + 2).start()

        def put(part, owner, side, value):
            if isinstance(part, int) and part >= levels:
                return
            stage[(chunk + 1) % 2, part, owner, piece, side] = value

        def dense(step, carry):
            width_dense(step, th_ref, tl_ref, v_ref, put)
            return carry

        lax.fori_loop(0, owners // 2, dense, 0)

    def finals_by(t):
        ready = t - jnp.maximum(here, last) - SLACK + 1
        late = jnp.minimum(jnp.maximum(t - (total - ahead) + 1, 0), 1)
        return jnp.minimum(jnp.maximum(ready - HOLD * (1 - late), 0), total)

    def begin(t, carry):
        start_forward(t)
        return carry

    lax.fori_loop(0, min(ahead, total), begin, 0)

    def step(t, carry):
        @pl.when(t + ahead < total)
        def _():
            start_forward(t + ahead)

        @when(t < total, active(t))
        def _():
            arrived(t).wait()
            others(t, recv_f).wait()
            columns(t)

        right = t - here - SLACK * jnp.minimum(here, 1)

        @when(right >= 0, right < total)
        def _():
            for q in range(depths - 1, 0, -1):
                @when(here > 0, q >= here, jnp.logical_or(here > 1, filled(right)))
                def _():
                    landed(right, q - here, recv_r.at[right, q - 1]).wait()
                    merge(right, q, q - here)

                @when(q > here, jnp.logical_or(here > 0, filled(right)))
                def _():
                    right_copy(right, q).start()

        left = t - last - SLACK * jnp.minimum(last, 1)

        @when(left >= 0, left < total)
        def _():
            for q in range(depths - 1):
                @when(last > 0, q <= here, jnp.logical_or(last > 1, filled(left)))
                def _():
                    landed(left, depths - here + q, recv_l.at[left, q]).wait()
                    merge(left, q, depths - here + q)

                @when(q < here, jnp.logical_or(last > 0, filled(left)))
                def _():
                    left_copy(left, q).start()

        def send_final(done, carry):
            final_own(done).start()
            for step in range(1, owners):
                final_copy(done, (me + step) % owners).start()
            return carry

        lax.fori_loop(finals_by(t - 1), finals_by(t), send_final, 0)

        group, piece = t // levels, t % levels
        for chunk in range(1, chunks):
            @when(group == chunk - 1, piece < pieces)
            def _():
                if chunk > 2:
                    @pl.when(piece == 0)
                    def _():
                        def free(part, carry):
                            @pl.when(active(part))
                            def _():
                                others((chunk - 2) * levels + part, send_f).wait()

                            return carry

                        lax.fori_loop(0, levels, free, 0)
                width_tile(chunk, piece)

        return carry

    lax.fori_loop(0, total + depths - 1 + SLACK, step, 0)

    def finish(t, carry):
        group = t // levels

        @when(active(t), jnp.logical_or(group == 0, group + 2 >= chunks))
        def _():
            others(t, send_f).wait()

        for q in range(1, depths):
            @when(q > here, jnp.logical_or(here > 0, filled(t)))
            def _():
                right_copy(t, q).wait_send()
        for q in range(depths - 1):
            @when(q < here, jnp.logical_or(last > 0, filled(t)))
            def _():
                left_copy(t, q).wait_send()
        final_own(t).wait()
        finals(t, send_b).wait()
        finals(t, recv_b).wait()
        return carry

    lax.fori_loop(0, total, finish, 0)


def line(variant, chunks, owners, depths, sent, field, scalars, *tables):
    outer, levels = VARIANTS[variant]
    total = chunks * levels
    block = LOW // depths
    pieces = LOW // owners
    vmem = pl.BlockSpec(memory_space=pltpu.VMEM)
    hbm = pl.BlockSpec(memory_space=pl.ANY)
    dma = pltpu.SemaphoreType.DMA
    tile = (2, PART, HIGH)
    return pl.pallas_call(
        functools.partial(line_kernel, chunks, owners, depths, outer, levels),
        in_specs=[pl.BlockSpec(memory_space=pltpu.SMEM)] + [vmem] * len(tables) + [hbm, hbm],
        out_specs=hbm,
        out_shape=jax.ShapeDtypeStruct((chunks * PARTS, owners) + tile, jnp.float32),
        scratch_shapes=[
            pltpu.VMEM((total, LOW) + tile, jnp.float32),
            pltpu.VMEM((total, depths + 1, block) + tile, jnp.float32),
            pltpu.VMEM((2, levels, owners, pieces) + tile, jnp.float32),
            pltpu.VMEM((2, 2, HIGH // 2, N), jnp.float32),
            pltpu.VMEM((owners, HIGH, 2 * HIGH), jnp.float32),
            pltpu.VMEM((LOW,) + tile, jnp.float32),
            dma((total,)), dma((total,)), dma((total,)),
            dma((total, depths - 1)), dma((total, depths - 1)),
            dma((total, depths - 1)), dma((total, depths - 1)),
            dma((total,)), dma((total,)), dma((total,)),
            dma((2,)),
        ],
        compiler_params=pltpu.CompilerParams(vmem_limit_bytes=LINE_VMEM, collective_id=1 + variant, has_side_effects=True),
    )(scalars, *tables, sent, field)


def gather_kernel(chunks, owners, levels_ref, in_ref, tr_ref, ti_ref, th_ref, tl_ref, out_ref, held_ref, work_ref, o_ref, in_sem, out_sem):
    levels = levels_ref[1]
    lines = 8

    def in_copy(chunk):
        some = pl.ds(chunk * PARTS, PARTS)
        return pltpu.make_async_copy(in_ref.at[some], held_ref.at[some], in_sem.at[chunk])

    def out_copy(step):
        rows = pl.ds(pl.multiple_of(step * lines, lines), lines)
        return pltpu.make_async_copy(o_ref.at[:, rows, :], out_ref.at[:, rows, :], out_sem.at[step])

    for chunk in range(chunks):
        in_copy(chunk).start()

    for chunk in range(chunks):
        in_copy(chunk).wait()

        def dense(owner, carry):
            k = owner * chunks + chunk
            sides = [
                jnp.concatenate([
                    jnp.where(part < levels, held_ref[chunk * PARTS + part, owner, side], 0.0) for part in range(PARTS)
                ], axis=0).T
                for side in range(2)
            ]
            high, low = split(jnp.concatenate(sides, axis=1))
            out = dot(high, th_ref[...]) + dot(low, th_ref[...]) + dot(high, tl_ref[...])
            real, imaginary = out[:, :HIGH], out[:, HIGH:]
            turn_real, turn_imaginary = tr_ref[pl.ds(k, 1), :], ti_ref[pl.ds(k, 1), :]
            work_ref[k, 0] = real * turn_real - imaginary * turn_imaginary
            work_ref[k, 1] = real * turn_imaginary + imaginary * turn_real
            return carry

        lax.fori_loop(0, owners, dense, 0, unroll=4)

    def body(step, carry):
        rows = pl.ds(pl.multiple_of(step * lines, lines), lines)
        values = [(work_ref[k, 0, rows, :], work_ref[k, 1, rows, :]) for k in range(LOW)]
        for j, (real, imaginary) in enumerate(butterfly(values, 1.0)):
            o_ref[0, rows, j * HIGH:(j + 1) * HIGH] = real
            o_ref[1, rows, j * HIGH:(j + 1) * HIGH] = imaginary
        out_copy(step).start()
        return carry

    lax.fori_loop(0, HIGH // lines, body, 0)

    def flush(step, carry):
        out_copy(step).wait()
        return carry

    lax.fori_loop(0, HIGH // lines, flush, 0)


def gather_width(parts, levels, chunks, owners, tables):
    vmem = pl.BlockSpec(memory_space=pltpu.VMEM)
    hbm = pl.BlockSpec(memory_space=pl.ANY)
    return pl.pallas_call(
        functools.partial(gather_kernel, chunks, owners),
        in_specs=[pl.BlockSpec(memory_space=pltpu.SMEM), hbm] + [vmem] * len(tables),
        out_specs=hbm,
        out_shape=jax.ShapeDtypeStruct((2, HIGH, N), jnp.float32),
        scratch_shapes=[
            pltpu.VMEM(parts.shape, jnp.float32),
            pltpu.VMEM((LOW, 2, HIGH, HIGH), jnp.float32),
            pltpu.VMEM((2, HIGH, N), jnp.float32),
            pltpu.SemaphoreType.DMA((chunks,)),
            pltpu.SemaphoreType.DMA((HIGH // 8,)),
        ],
        compiler_params=pltpu.CompilerParams(vmem_limit_bytes=VMEM_LIMIT),
        name="gather",
    )(levels, parts, *tables)


def fused(target, depth_index, band_mask):
    owners, depths = lax.axis_size("rows"), lax.axis_size("depth")
    chunks = LOW // owners
    field = target.reshape(target.shape[1:])
    scale = 1.0 / math.sqrt(N)
    forward, backward = dense_table(-1.0), dense_table(1.0)
    order = both(slots())
    turn = twiddles(-1.0, scale)
    turn_back = twiddles(1.0, scale / math.sqrt(depths))
    wide = halves(forward[order])
    sent, scalars, choice = spread_width(field, depth_index, band_mask, chunks, owners, depths, turn + wide)
    choices = [functools.partial(line, i, chunks, owners, depths) for i in range(len(VARIANTS))]
    tables = turn + wide + halves(forward.T) + halves(backward.T)
    parts = lax.switch(choice[0], choices, sent, field, scalars, *tables)
    return gather_width(parts, choice, chunks, owners, turn_back + halves(backward.T[order]))


def solution(mesh):
    in_specs = (P("depth", None, "rows", None), P("depth"), P("depth", None, None))
    out_specs = P(None, ("depth", "rows"), None)
    step = jax.shard_map(local, mesh=mesh, in_specs=in_specs, out_specs=out_specs, check_vma=False)
    if mesh.shape["rows"] * mesh.shape["depth"] == LOW and mesh.shape["depth"] > 1:
        return jax.shard_map(fused, mesh=mesh, in_specs=in_specs, out_specs=out_specs, check_vma=False)
    return step
```
